256 devices in a mesh: src: 32 (over y_lo, z, core), tgt: 8 (over x, y_hi).
Axes of the slice: x: 4, y: 4 (y_hi: 2, y_lo: 2; y = y_hi * 2 + y_lo), z: 8, core: 2. Of those that a mesh axis runs over, the one named last changes fastest.
Arguments:
- atom_feats: bfloat16 [2048, 3200], P(('src', 'tgt')), may hold values from -6 to 6
- positions: float32 [3, 2048], P(None, ('src', 'tgt')), may hold values from 0 to 1
- edge_src: int32 [262144], P(('src', 'tgt')), may hold values from 0 to 63
- edge_tgt: int32 [262144], P(('src', 'tgt')), may hold values from 0 to 255
- edge_angle: float32 [262144], P(('src', 'tgt')), may hold values from -3.140625 to 3.140625
- edge_scale: float32 [262144], P(('src', 'tgt')), may hold values from 0.1 to 1
- edge_count: int32 [32, 8], replicated, may hold values from 1 to 1024, as said below
- k_index: int32 [3, 2048], replicated, may hold values from -6 to 6
- k_filter: float32 [2048, 128], replicated, may hold values from -6 to 6
- weight_zero: bfloat16 [2, 640, 640], replicated, may hold values from -0.25 to 0.25
- weight_first: bfloat16 [2, 2, 512, 512], replicated, may hold values from -0.1875 to 0.1875
- weight_second: bfloat16 [2, 2, 384, 384], replicated, may hold values from -0.21875 to 0.21875
- weight_third: bfloat16 [2, 2, 256, 256], replicated, may hold values from -0.25 to 0.25
- weight_fourth: bfloat16 [2, 2, 128, 128], replicated, may hold values from -0.375 to 0.375
Outputs:
- edge_update: bfloat16 [2048, 3200], P(('tgt', 'src'))
- long_range: float32 [2048, 128], P(('src', 'tgt'))
The draws below stay inside these ranges and needn't reach their ends.
Inputs may be any that keep to these rules, and one draw needn't show every extreme that they name: `edge_count`: live edge slots of tile (s, t); in every draw some tile is full with 1024.
All inputs are finite; a program needn't handle non-finite values.
Results may differ from the reference program's by a relative error of at most 0.0047.
Values may be sent and summed in bfloat16 or wider, within the bound.
No kernel may reach another device: no remote copies, remote signals or barrier semaphores. Data moves between devices by JAX's collectives and lax.ppermute only.
A program may use at most 64 MiB of HBM per device.

```python
import math
import jax
import jax.numpy as jnp
from jax import lax

C = 128
LMAX = 4
FEATS = 3200
EDGE_CAP = 1024
KVECS = 2048
SRC_GROUPS = 32
TGT_GROUPS = 8
SRC_BLK = 64
TGT_BLK = 256
ATOMS = 2048
EDGES = 262144
N_TGT = 8
DEVICES = 256


def draw_edge_count(key, part):
    base_key = jax.random.fold_in(key, 11)
    full_key = jax.random.fold_in(key, 12)
    tiles = SRC_GROUPS * TGT_GROUPS
    counts = jax.random.randint(base_key, (tiles,), EDGE_CAP // 8, EDGE_CAP // 2 + 1)
    chosen = jax.random.randint(full_key, (), 0, tiles)
    counts = jnp.where(jnp.arange(tiles) == chosen, EDGE_CAP, counts)
    return counts.reshape(SRC_GROUPS, TGT_GROUPS).astype(jnp.int32)


def with_ends(array, rng, low, high):
    index_at = [jax.random.randint(jax.random.fold_in(rng, axis), (), 0, length) for axis, length in enumerate(array.shape)]
    main_axis = array.shape.index(max(array.shape))
    beside = index_at[:main_axis] + [(index_at[main_axis] + 1) % array.shape[main_axis]] + index_at[main_axis + 1:]
    return array.at[tuple(index_at)].set(low).at[tuple(beside)].set(high)


def block_scale(key, dims, shards, smallest, top_value):
    def one(dim, parts):
        heights = jax.random.uniform(jax.random.fold_in(jax.random.fold_in(key, 6), dim), (parts,), jnp.float32, smallest / len(shards), top_value / len(shards))
        return jnp.repeat(jnp.exp(heights), dims[dim] // parts).reshape((-1,) + (1,) * (len(dims) - dim - 1))

    loudness = one(*shards[0])
    for cut in shards[1:]:
        loudness = loudness * one(*cut)
    return loudness


def gaussian(own_key, extent, scale, reach, shards=(), held_as=jnp.bfloat16):
    array = scale * jax.random.normal(own_key, extent, jnp.float32)
    if shards:
        array = array * block_scale(own_key, extent, shards, -0.22, 0.18)
    return jnp.clip(array, -reach, reach).astype(held_as)


def setup_inputs(seed: int = 0) -> dict:
    seeds = jax.random.split(jax.random.key(seed), 15)
    return {
        "atom_feats": gaussian(seeds[0], (ATOMS, FEATS), 1.0, 6.0, ((0, 256),)),
        "positions": jnp.clip(1.0 * jax.random.uniform(seeds[1], (3, ATOMS), jnp.float32) ** block_scale(seeds[1], (3, ATOMS), ((1, 256),), -0.2, 0.2), 0.0, 1.0),
        "edge_src": with_ends(jax.random.randint(seeds[2], (EDGES,), 0, SRC_BLK), jax.random.fold_in(seeds[2], 1), 0, SRC_BLK - 1).astype(jnp.int32),
        "edge_tgt": with_ends(jax.random.randint(seeds[3], (EDGES,), 0, TGT_BLK), jax.random.fold_in(seeds[3], 1), 0, TGT_BLK - 1).astype(jnp.int32),
        "edge_angle": jnp.clip(jax.random.uniform(seeds[4], (EDGES,), jnp.float32, -3.140625, 3.140625), -3.140625, 3.140625),
        "edge_scale": jnp.clip(jnp.exp(math.log(1.0) - 2.3025851 * jax.random.uniform(seeds[5], (EDGES,), jnp.float32) ** block_scale(seeds[5], (EDGES,), ((0, 256),), -0.2, 0.2)), 0.1, 1.0),
        "edge_count": draw_edge_count(jax.random.fold_in(seeds[14], 71), 0),
        "k_index": with_ends(jax.random.randint(seeds[7], (3, KVECS), -6, 7), jax.random.fold_in(seeds[7], 1), -6, 6).astype(jnp.int32),
        "k_filter": gaussian(seeds[8], (KVECS, C), 1.0, 6.0, (), jnp.float32),
        "weight_zero": gaussian(seeds[9], (2, (LMAX + 1) * C, (LMAX + 1) * C), ((LMAX + 1) * C) ** -0.5, 0.25),
        "weight_first": gaussian(seeds[10], (2, 2, LMAX * C, LMAX * C), (2 * LMAX * C) ** -0.5, 0.1875),
        "weight_second": gaussian(seeds[11], (2, 2, (LMAX - 1) * C, (LMAX - 1) * C), (2 * (LMAX - 1) * C) ** -0.5, 0.21875),
        "weight_third": gaussian(seeds[12], (2, 2, (LMAX - 2) * C, (LMAX - 2) * C), (2 * (LMAX - 2) * C) ** -0.5, 0.25),
        "weight_fourth": gaussian(seeds[13], (2, 2, (LMAX - 3) * C, (LMAX - 3) * C), (2 * (LMAX - 3) * C) ** -0.5, 0.375),
    }


def rotate(values, angles, handed):
    pieces = [values[:, :(LMAX + 1) * C]]
    offset = (LMAX + 1) * C
    for degree in range(1, LMAX + 1):
        columns = (LMAX + 1 - degree) * C
        cosine = jnp.cos(degree * angles)[:, None]
        sine_part = handed * jnp.sin(degree * angles)[:, None]
        leading = values[:, offset:offset + columns]
        trailing = values[:, offset + columns:offset + 2 * columns]
        pieces.append(cosine * leading + sine_part * trailing)
        pieces.append(cosine * trailing - sine_part * leading)
        offset += 2 * columns
    return jnp.concatenate(pieces, axis=1)

def pair_matrix(weights, conv_index):
    upper_half = jnp.concatenate([weights[conv_index, 0], weights[conv_index, 1]], axis=1)
    lower_half = jnp.concatenate([-weights[conv_index, 1], weights[conv_index, 0]], axis=1)
    return jnp.concatenate([upper_half, lower_half], axis=0)

def convolve(inputs, matrices):
    outputs = []
    offset = 0
    for matrix in matrices:
        height = matrix.shape[0]
        outputs.append(jnp.dot(inputs[:, offset:offset + height], matrix, preferred_element_type=jnp.float32))
        offset += height
    return jnp.concatenate(outputs, axis=1)

def edge_message(edge_rows, angles, scales, matrices_one, matrices_two):
    turned = rotate(edge_rows.astype(jnp.float32), angles, 1.0).astype(jnp.bfloat16)
    hidden = jax.nn.gelu(convolve(turned, matrices_one), approximate=False).astype(jnp.bfloat16)
    second = convolve(hidden, matrices_two)
    return rotate(second, angles, -1.0) * scales[:, None]

def reference(atom_feats, positions, edge_src, edge_tgt, edge_angle, edge_scale, edge_count, k_index, k_filter, weight_zero, weight_first, weight_second, weight_third, weight_fourth):
    sections = []
    for conv_index in (0, 1):
        sections.append([weight_zero[conv_index]] + [pair_matrix(weights, conv_index) for weights in (weight_first, weight_second, weight_third, weight_fourth)])
    slot_ids = jnp.arange(EDGE_CAP, dtype=jnp.int32)

    def add_tile(tile_index, totals):
        tile_index = tile_index.astype(jnp.int32)
        source_group = tile_index // N_TGT
        target_group = tile_index % N_TGT
        source_block = lax.dynamic_slice_in_dim(atom_feats, (source_group * SRC_BLK).astype(jnp.int32), SRC_BLK, 0)
        first_slot = (tile_index * EDGE_CAP).astype(jnp.int32)
        sources = lax.dynamic_slice_in_dim(edge_src, first_slot, EDGE_CAP)
        targets = lax.dynamic_slice_in_dim(edge_tgt, first_slot, EDGE_CAP)
        angles = lax.dynamic_slice_in_dim(edge_angle, first_slot, EDGE_CAP)
        scales = lax.dynamic_slice_in_dim(edge_scale, first_slot, EDGE_CAP)
        live_mask = (slot_ids < edge_count[source_group, target_group]).astype(jnp.float32)
        edge_rows = jnp.take(source_block, sources, axis=0)
        messages = edge_message(edge_rows, angles, scales, sections[0], sections[1]) * live_mask[:, None]
        partial_value = jax.ops.segment_sum(messages, targets, num_segments=TGT_BLK)
        row_start = (target_group * TGT_BLK).astype(jnp.int32)
        current = lax.dynamic_slice_in_dim(totals, row_start, TGT_BLK, 0)
        return lax.dynamic_update_slice_in_dim(totals, current + partial_value, row_start, 0)
    totals = lax.fori_loop(0, DEVICES, add_tile, jnp.zeros((ATOMS, FEATS), jnp.float32))
    edge_update = totals.astype(jnp.bfloat16)
    k_float = k_index.astype(jnp.float32)
    phase = 2.0 * math.pi * (positions[0][:, None] * k_float[0][None, :] + positions[1][:, None] * k_float[1][None, :] + positions[2][:, None] * k_float[2][None, :])
    cos_table = jnp.cos(phase)
    sin_table = jnp.sin(phase)
    charges = atom_feats[:, :C].astype(jnp.float32)
    factors_cos = jnp.dot(cos_table.T, charges, precision=lax.Precision.HIGHEST, preferred_element_type=jnp.float32)
    factors_sin = jnp.dot(sin_table.T, charges, precision=lax.Precision.HIGHEST, preferred_element_type=jnp.float32)
    summed = jnp.dot(cos_table, k_filter * factors_cos, precision=lax.Precision.HIGHEST, preferred_element_type=jnp.float32) + jnp.dot(sin_table, k_filter * factors_sin, precision=lax.Precision.HIGHEST, preferred_element_type=jnp.float32)
    long_range = summed * (1.0 / math.sqrt(ATOMS * KVECS))
    return (edge_update, long_range)
```

```python
import math

import jax
import jax.numpy as jnp
from jax import lax
from jax.experimental import pallas as pl
from jax.experimental.pallas import tpu as pltpu
from jax.sharding import Mesh
from jax.sharding import PartitionSpec as P

Y, ZH, R, TGT = 2, 4, 4, 8
SRC_AXES = ("y", "zh", "r")
GROUP_AXES = ("y", "r", "tgt")
ALL_AXES = ("y", "zh", "r", "tgt")
SRC = Y * ZH * R
SLICES = Y * R
LANES = 128
ROWS = 8
BLOCKS = 25
CH = LANES // SLICES
COLS = BLOCKS * CH
STEP = 256
POS_LANE = 16
F32 = jnp.float32
BF16 = jnp.bfloat16
VMEM_LIMIT = 48 << 20


def order_spans():
    spans = [(0, 5)]
    offset = 5
    for order in range(1, 5):
        spans.append((offset, 5 - order))
        offset += 2 * (5 - order)
    return spans


SPANS = order_spans()


def sincos_turns(turns):
    part = turns - jnp.floor(turns + 0.5)
    x = part * math.pi
    x2 = x * x
    s = -1.0 / math.factorial(11)
    for k in (9, 7, 5, 3):
        s = s * x2 + (1.0 if k % 4 == 1 else -1.0) / math.factorial(k)
    s = x + x * (x2 * s)
    c = 1.0 / math.factorial(12)
    for k in (10, 8, 6, 4, 2):
        c = c * x2 + (1.0 if k % 4 == 0 else -1.0) / math.factorial(k)
    c = 1.0 + x2 * c
    return 1.0 - 2.0 * s * s, 2.0 * s * c


def split2(value):
    high = value.astype(BF16)
    return high, (value - high.astype(F32)).astype(BF16)


def position_tile(pos_ref):
    row_ids = lax.broadcasted_iota(jnp.int32, (ROWS, ROWS), 0)
    col_ids = lax.broadcasted_iota(jnp.int32, (ROWS, ROWS), 1)
    lane = lax.broadcasted_iota(jnp.int32, (ROWS, LANES), 1)
    tile = jnp.zeros((ROWS, LANES), F32)
    for axis in range(3):
        spread = jnp.broadcast_to(pos_ref[axis : axis + 1, :], (ROWS, ROWS))
        rest = jnp.sum(jnp.where(row_ids == col_ids, spread, 0.0), axis=1, keepdims=True)
        for part in range(3):
            piece = rest.astype(BF16).astype(F32)
            rest = rest - piece
            tile = jnp.where(lane == POS_LANE + 3 * axis + part, piece, tile)
    return tile


def edge_pack_kernel(count_ref, src_ref, tgt_ref, angle_ref, scale_ref, pos_ref, out_ref):
    group = (lax.axis_index("y") * ZH + lax.axis_index("zh")) * R + lax.axis_index("r")
    count = count_ref[group, lax.axis_index("tgt")]
    slot = lax.broadcasted_iota(jnp.int32, (ROWS, LANES), 0) * LANES + lax.broadcasted_iota(
        jnp.int32, (ROWS, LANES), 1
    )
    angle = angle_ref[...]
    angle_high = angle.astype(BF16).astype(F32)
    tiles = (
        src_ref[...].astype(F32),
        jnp.where(slot < count, tgt_ref[...], SRC * ROWS).astype(F32),
        angle_high,
        angle - angle_high,
        scale_ref[...],
        position_tile(pos_ref),
    )
    for index, tile in enumerate(tiles):
        out_ref[:, index, :, :] = jnp.broadcast_to(tile.astype(BF16)[None], (SRC, ROWS, LANES))


def pair_product(stacked, weight_ref, order):
    first = jnp.dot(stacked, weight_ref[0, 0], preferred_element_type=F32)
    second = jnp.dot(stacked, weight_ref[0, 1], preferred_element_type=F32)
    lead = jnp.zeros((ROWS, first.shape[1]), F32)
    trail = lead
    for base in range(0, stacked.shape[0], 2 * ROWS):
        lead = lead + (first[base : base + ROWS] - second[base + ROWS : base + 2 * ROWS])
        trail = trail + (second[base : base + ROWS] + first[base + ROWS : base + 2 * ROWS])
    return lead, trail


def first_conv_kernel(feats_ref, pos_ref, w0, w1, w2, w3, w4, out_ref, conv_ref):
    x = feats_ref[...].astype(F32)
    width = SPANS[0][1] * LANES
    conv_ref[:, :width] = jnp.dot(x[:, :width].astype(BF16), w0[0], preferred_element_type=F32)
    for order, weight in zip(range(1, 5), (w1, w2, w3, w4)):
        offset, blocks = SPANS[order]
        start, width = offset * LANES, blocks * LANES
        stacked = jnp.concatenate([x[:, start : start + width], x[:, start + width : start + 2 * width]], axis=0)
        lead, trail = pair_product(stacked.astype(BF16), weight, order)
        conv_ref[:, start : start + width] = lead
        conv_ref[:, start + width : start + 2 * width] = trail
    lane = lax.broadcasted_iota(jnp.int32, (ROWS, LANES), 1)
    place = lane // CH
    pos = position_tile(pos_ref)
    for tile_index in range(4):
        for piece in range(SLICES):
            tile = pos if tile_index == 3 else jnp.zeros((ROWS, LANES), F32)
            for within in range(min(8, BLOCKS - 8 * tile_index)):
                block = 8 * tile_index + within
                moved = conv_ref[:, block * LANES : (block + 1) * LANES]
                if within != piece:
                    moved = pltpu.roll(moved, (CH * (within - piece)) % LANES, 1)
                tile = jnp.where(place == within, moved * math.sqrt(0.5), tile)
            out_ref[piece * TGT : (piece + 1) * TGT, tile_index, :, :] = jnp.broadcast_to(
                tile.astype(BF16)[None], (TGT, ROWS, LANES)
            )
    out_ref[:, 4, :, :] = jnp.broadcast_to(feats_ref[:, :LANES][None], (SLICES * TGT, ROWS, LANES))


def dot_first(left, right):
    return lax.dot_general(left, right, (((0,), (0,)), ((), ())), preferred_element_type=F32)


def main_kernel(
    count_ref,
    feats_ref,
    edges_ref,
    kidx_ref,
    kfilter_hbm,
    out_ref,
    kfilter_ref,
    src_ref,
    tgt_ref,
    coef_ref,
    xt_ref,
    rows_ref,
    yt_ref,
    acc_ref,
    filter_sem,
):
    zone = lax.axis_index("zh")
    piece = lax.axis_index("y") * R + lax.axis_index("r")
    target_group = lax.axis_index("tgt")
    kslice = SRC * ROWS
    k_start = pl.multiple_of(piece * kslice, kslice)
    fetch = pltpu.make_async_copy(kfilter_hbm.at[pl.ds(k_start, kslice), :], kfilter_ref, filter_sem)
    fetch.start()

    for tile in range(SLICES):
        source = (tile // R) * (ZH * R) + zone * R + tile % R
        rows = pl.ds(ROWS * tile, ROWS)
        src_ref[rows, :] = edges_ref[source, 0, :, :].astype(F32)
        tgt_ref[rows, :] = edges_ref[source, 1, :, :].astype(F32)
        angle = edges_ref[source, 2, :, :].astype(F32) + edges_ref[source, 3, :, :].astype(F32)
        scale = edges_ref[source, 4, :, :].astype(F32) * math.sqrt(0.5)
        c1, s1 = sincos_turns(angle * (0.5 / math.pi))
        c, s = c1, s1
        coef_ref[16, rows, :] = scale
        for order in range(4):
            if order:
                c, s = c * c1 - s * s1, s * c1 + c * s1
            coef_ref[4 * order, rows, :] = c
            coef_ref[4 * order + 1, rows, :] = s
            coef_ref[4 * order + 2, rows, :] = scale * c
            coef_ref[4 * order + 3, rows, :] = scale * s

    acc_ref[...] = jnp.zeros_like(acc_ref)
    src_ids = lax.broadcasted_iota(jnp.int32, (TGT * ROWS, STEP), 0).astype(F32)
    tgt_ids = lax.broadcasted_iota(jnp.int32, (SRC * ROWS, STEP), 0).astype(F32)

    def one_tile(tile, carry):
        source = (tile // R) * (ZH * R) + zone * R + tile % R
        count = count_ref[source, target_group]
        for index in range(4):
            block = feats_ref[pl.ds(tile * TGT, TGT), index, :, :].astype(F32).reshape(TGT * ROWS, LANES)
            width = min(LANES, COLS - index * LANES)
            xt_ref[index * LANES : index * LANES + width, :] = block.T[:width].astype(BF16)

        def one_step(step, inner):
            row = tile * ROWS + step * (STEP // LANES)

            def lanes_of(ref, *lead):
                return jnp.concatenate(
                    [ref[(*lead, pl.ds(row + part, 1), slice(None))] for part in range(STEP // LANES)], axis=1
                )

            one_src = (src_ids == lanes_of(src_ref)).astype(F32).astype(BF16)
            rows_ref[...] = jnp.dot(xt_ref[...], one_src, preferred_element_type=F32)
            width = SPANS[0][1] * CH
            gathered = rows_ref[:width, :]
            hidden = gathered + gathered * lax.erf(gathered)
            yt_ref[:width, :] = (hidden * lanes_of(coef_ref, 16)).astype(BF16)
            for order in range(1, 5):
                offset, blocks = SPANS[order]
                cos_in, sin_in, cos_out, sin_out = (lanes_of(coef_ref, 4 * (order - 1) + part) for part in range(4))
                for block in range(blocks):
                    low = (offset + block) * CH
                    high = low + blocks * CH
                    lead, trail = rows_ref[low : low + CH, :], rows_ref[high : high + CH, :]
                    lead, trail = cos_in * lead + sin_in * trail, cos_in * trail - sin_in * lead
                    lead, trail = lead + lead * lax.erf(lead), trail + trail * lax.erf(trail)
                    yt_ref[low : low + CH, :] = (cos_out * lead - sin_out * trail).astype(BF16)
                    yt_ref[high : high + CH, :] = (cos_out * trail + sin_out * lead).astype(BF16)
            one_tgt = (tgt_ids == lanes_of(tgt_ref)).astype(F32).astype(BF16)
            acc_ref[:, :COLS] += lax.dot_general(
                one_tgt, yt_ref[...], (((1,), (1,)), ((), ())), preferred_element_type=F32
            )
            return inner

        return lax.fori_loop(0, (count + STEP - 1) // STEP, one_step, carry)

    lax.fori_loop(0, SLICES, one_tile, 0)
    for index in range(4):
        out_ref[:, index, :, :] = (
            acc_ref[:, index * LANES : (index + 1) * LANES].reshape(SRC, ROWS, LANES).astype(BF16)
        )

    row_ids = lax.broadcasted_iota(jnp.int32, (LANES, kslice), 0)
    k_rows = kidx_ref[:, pl.ds(k_start, kslice)].astype(F32)
    k_table = jnp.zeros((LANES, kslice), F32)
    for axis in range(3):
        start = POS_LANE + 3 * axis
        k_table = jnp.where((row_ids >= start) & (row_ids < start + 3), k_rows[axis : axis + 1, :], k_table)
    k_table = k_table.astype(BF16)
    atoms = SLICES * TGT * ROWS
    charges = feats_ref[:, 4, :, :].reshape(atoms, LANES)
    turns = jnp.dot(feats_ref[:, 3, :, :].reshape(atoms, LANES), k_table, preferred_element_type=F32)
    tables = sincos_turns(turns)
    own_turns = jnp.dot(edges_ref[:, 5, :, :].reshape(kslice, LANES), k_table, preferred_element_type=F32)
    own_tables = sincos_turns(own_turns)
    fetch.wait()
    total = jnp.zeros((kslice, LANES), F32)
    for table, own_table in zip(tables, own_tables):
        high, low = split2(table)
        factors = kfilter_ref[...] * (dot_first(high, charges) + dot_first(low, charges))
        own_high, own_low = split2(own_table)
        factors_high, factors_low = split2(factors)
        total = total + jnp.dot(own_high, factors_high, preferred_element_type=F32)
        total = total + jnp.dot(own_low, factors_high, preferred_element_type=F32)
        total = total + jnp.dot(own_high, factors_low, preferred_element_type=F32)
    out_ref[:, 4, :, :] = total.reshape(SRC, ROWS, LANES).astype(BF16)


def last_conv_kernel(norm, parts_ref, w0, w1, w2, w3, w4, update_ref, long_ref, conv_ref):
    total = jnp.zeros((ROWS, LANES), F32)
    for source in range(SRC):
        total = total + parts_ref[source, 4, :, :].astype(F32)
    long_ref[...] = total * norm
    place = lax.broadcasted_iota(jnp.int32, (ROWS, LANES), 1) // CH
    for index in range(4):
        sums = []
        for piece in range(SLICES):
            total = jnp.zeros((ROWS, LANES), F32)
            for zone in range(ZH):
                source = (piece // R) * (ZH * R) + zone * R + piece % R
                total = total + parts_ref[source, index, :, :].astype(F32)
            sums.append(total)
        for within in range(min(8, BLOCKS - 8 * index)):
            block = 8 * index + within
            tile = jnp.zeros((ROWS, LANES), F32)
            for piece in range(SLICES):
                moved = sums[piece]
                if within != piece:
                    moved = pltpu.roll(moved, (CH * (piece - within)) % LANES, 1)
                tile = jnp.where(place == piece, moved, tile)
            conv_ref[:, block * LANES : (block + 1) * LANES] = tile
    width = SPANS[0][1] * LANES
    value = conv_ref[:, :width]
    rounded = value.astype(BF16).astype(F32)
    stacked = jnp.concatenate([rounded, value - rounded], axis=0).astype(BF16)
    product = jnp.dot(stacked, w0[0], preferred_element_type=F32)
    update_ref[:, :width] = (product[:ROWS] + product[ROWS:]).astype(BF16)
    for order, weight in zip(range(1, 5), (w1, w2, w3, w4)):
        offset, blocks = SPANS[order]
        start, width = offset * LANES, blocks * LANES
        lead, trail = conv_ref[:, start : start + width], conv_ref[:, start + width : start + 2 * width]
        lead_high, trail_high = lead.astype(BF16).astype(F32), trail.astype(BF16).astype(F32)
        stacked = jnp.concatenate([lead_high, trail_high, lead - lead_high, trail - trail_high], axis=0)
        lead, trail = pair_product(stacked.astype(BF16), weight, order)
        update_ref[:, start : start + width] = lead.astype(BF16)
        update_ref[:, start + width : start + 2 * width] = trail.astype(BF16)


def whole(shape):
    return pl.BlockSpec(shape, lambda i: (0,) * len(shape))


def weight_specs(weights, conv_index):
    specs = []
    for weight in weights:
        block = (1,) + weight.shape[1:]
        specs.append(pl.BlockSpec(block, lambda i, rank=len(block): (conv_index,) + (0,) * (rank - 1)))
    return specs


def params():
    return pltpu.CompilerParams(vmem_limit_bytes=VMEM_LIMIT)


def body(
    atom_feats,
    positions,
    edge_src,
    edge_tgt,
    edge_angle,
    edge_scale,
    edge_count,
    k_index,
    k_filter,
    *weights,
):
    slots = edge_src.shape[0]
    columns = atom_feats.shape[1]
    tile_shape = (ROWS, slots // ROWS)
    smem = pl.BlockSpec(memory_space=pltpu.SMEM)
    edges_out = (SRC, 6, ROWS, LANES)
    edges = pl.pallas_call(
        edge_pack_kernel,
        grid=(1,),
        out_shape=jax.ShapeDtypeStruct(edges_out, BF16),
        in_specs=[smem] + [whole(tile_shape)] * 4 + [whole(positions.shape)],
        out_specs=whole(edges_out),
        compiler_params=params(),
        name="edge_pack",
    )(edge_count, *(value.reshape(tile_shape) for value in (edge_src, edge_tgt, edge_angle, edge_scale)), positions)
    edges = lax.all_to_all(edges, SRC_AXES, 0, 0)

    feats_out = (SLICES * TGT, 5, ROWS, LANES)
    feats = pl.pallas_call(
        first_conv_kernel,
        grid=(1,),
        out_shape=jax.ShapeDtypeStruct(feats_out, BF16),
        in_specs=[whole(atom_feats.shape), whole(positions.shape)] + weight_specs(weights, 0),
        out_specs=whole(feats_out),
        scratch_shapes=[pltpu.VMEM((ROWS, columns), F32)],
        compiler_params=params(),
        name="first_conv",
    )(atom_feats, positions, *weights)
    feats = lax.all_to_all(feats, GROUP_AXES, 0, 0)

    parts_out = (SRC, 5, ROWS, LANES)
    kslice = SRC * ROWS
    parts = pl.pallas_call(
        main_kernel,
        grid=(1,),
        out_shape=jax.ShapeDtypeStruct(parts_out, BF16),
        in_specs=[
            smem,
            whole(feats_out),
            whole(edges_out),
            whole(k_index.shape),
            pl.BlockSpec(memory_space=pl.ANY),
        ],
        out_specs=whole(parts_out),
        scratch_shapes=[
            pltpu.VMEM((kslice, LANES), F32),
            pltpu.VMEM((SLICES * ROWS, LANES), F32),
            pltpu.VMEM((SLICES * ROWS, LANES), F32),
            pltpu.VMEM((17, SLICES * ROWS, LANES), F32),
            pltpu.VMEM((COLS, TGT * ROWS), BF16),
            pltpu.VMEM((COLS, STEP), F32),
            pltpu.VMEM((COLS, STEP), BF16),
            pltpu.VMEM((kslice, 4 * LANES), F32),
            pltpu.SemaphoreType.DMA,
        ],
        compiler_params=params(),
        name="edge_sums",
    )(edge_count, feats, edges, k_index, k_filter)
    parts = lax.all_to_all(parts, SRC_AXES, 0, 0)

    norm = 1.0 / math.sqrt(SRC * TGT * ROWS * k_filter.shape[0])
    return pl.pallas_call(
        lambda *refs: last_conv_kernel(norm, *refs),
        grid=(1,),
        out_shape=(
            jax.ShapeDtypeStruct((ROWS, columns), BF16),
            jax.ShapeDtypeStruct((ROWS, LANES), F32),
        ),
        in_specs=[whole(parts_out)] + weight_specs(weights, 1),
        out_specs=(whole((ROWS, columns)), whole((ROWS, LANES))),
        scratch_shapes=[pltpu.VMEM((ROWS, columns), F32)],
        compiler_params=params(),
        name="last_conv",
    )(parts, *weights)


def solution(mesh):
    fine = Mesh(mesh.devices.reshape(Y, ZH, R, TGT), ALL_AXES)
    return jax.shard_map(
        body,
        mesh=fine,
        in_specs=(P(ALL_AXES, None), P(None, ALL_AXES)) + (P(ALL_AXES),) * 4 + (P(),) * 8,
        out_specs=(P(("tgt",) + SRC_AXES, None), P(ALL_AXES, None)),
        check_vma=False,
    )
```

```python
import math

import jax
import jax.numpy as jnp
from jax import lax
from jax.experimental import pallas as pl
from jax.experimental.pallas import tpu as pltpu
from jax.sharding import Mesh
from jax.sharding import PartitionSpec as P

Y, ZH, R, TGT = 2, 4, 4, 8
SRC_AXES = ("y", "zh", "r")
ALL_AXES = ("y", "zh", "r", "tgt")
SRC = Y * ZH * R
SLICES = Y * R
LANES = 128
ROWS = 8
BLOCKS = 25
CH = LANES // SLICES
COLS = BLOCKS * CH
STEP = 256
POS_LANE = 16
COST = {
    "first": pl.CostEstimate(flops=50_000_000, transcendentals=0, bytes_accessed=3_000_000),
    "spread": pl.CostEstimate(flops=0, transcendentals=0, bytes_accessed=800_000),
    "edge_sums": pl.CostEstimate(flops=8_000_000_000, transcendentals=1_500_000, bytes_accessed=2_000_000),
    "last_conv": pl.CostEstimate(flops=100_000_000, transcendentals=0, bytes_accessed=3_200_000),
}
F32 = jnp.float32
BF16 = jnp.bfloat16


def order_spans():
    spans = [(0, 5)]
    offset = 5
    for order in range(1, 5):
        spans.append((offset, 5 - order))
        offset += 2 * (5 - order)
    return spans


SPANS = order_spans()


def sincos_turns(turns):
    part = turns - jnp.floor(turns + 0.5)
    x = part * math.pi
    x2 = x * x
    s = 1.0 / math.factorial(9)
    for k in (7, 5, 3):
        s = s * x2 + (1.0 if k % 4 == 1 else -1.0) / math.factorial(k)
    s = x + x * (x2 * s)
    c = -1.0 / math.factorial(10)
    for k in (8, 6, 4, 2):
        c = c * x2 + (1.0 if k % 4 == 0 else -1.0) / math.factorial(k)
    c = 1.0 + x2 * c
    return 1.0 - 2.0 * s * s, 2.0 * s * c


def split2(value):
    high = value.astype(BF16)
    return high, (value - high.astype(F32)).astype(BF16)


def position_tile(pos_ref):
    row_ids = lax.broadcasted_iota(jnp.int32, (ROWS, ROWS), 0)
    col_ids = lax.broadcasted_iota(jnp.int32, (ROWS, ROWS), 1)
    lane = lax.broadcasted_iota(jnp.int32, (ROWS, LANES), 1)
    tile = jnp.zeros((ROWS, LANES), F32)
    for axis in range(3):
        spread = jnp.broadcast_to(pos_ref[axis : axis + 1, :], (ROWS, ROWS))
        rest = jnp.sum(jnp.where(row_ids == col_ids, spread, 0.0), axis=1, keepdims=True)
        for part in range(3):
            piece = rest.astype(BF16).astype(F32)
            rest = rest - piece
            tile = jnp.where(lane == POS_LANE + 3 * axis + part, piece, tile)
    return tile


def edge_tiles(count_ref, src_ref, tgt_ref, angle_ref, scale_ref):
    group = (lax.axis_index("y") * ZH + lax.axis_index("zh")) * R + lax.axis_index("r")
    count = count_ref[lax.axis_index("tgt"), group]
    slot = lax.broadcasted_iota(jnp.int32, (ROWS, LANES), 0) * LANES + lax.broadcasted_iota(
        jnp.int32, (ROWS, LANES), 1
    )
    angle = angle_ref[...]
    angle_high = angle.astype(BF16).astype(F32)
    return (
        src_ref[...].astype(F32),
        jnp.where(slot < count, tgt_ref[...], SRC * ROWS).astype(F32),
        angle_high,
        angle - angle_high,
        scale_ref[...],
    )


def pair_product(stacked, weight_ref):
    first = jnp.dot(stacked, weight_ref[0], preferred_element_type=F32)
    second = jnp.dot(stacked, weight_ref[1], preferred_element_type=F32)
    lead = jnp.zeros((ROWS, first.shape[1]), F32)
    trail = lead
    for base in range(0, stacked.shape[0], 2 * ROWS):
        lead = lead + (first[base : base + ROWS] - second[base + ROWS : base + 2 * ROWS])
        trail = trail + (second[base : base + ROWS] + first[base + ROWS : base + 2 * ROWS])
    return lead, trail


def first_kernel(count_ref, *refs):
    sources, kfilter_hbm, (out_ref, kslice_ref) = refs[:11], refs[11], refs[12:14]
    held, (conv_ref, sems) = refs[14:25], refs[25:]
    copies = [
        pltpu.make_async_copy(source if index < 6 else source.at[0], to, sems.at[index])
        for index, (source, to) in enumerate(zip(sources, held))
    ]
    for copy in copies:
        copy.start()
    kslice = kslice_ref.shape[0]
    k_start = pl.multiple_of((lax.axis_index("y") * R + lax.axis_index("r")) * kslice, kslice)
    copies.append(pltpu.make_async_copy(kfilter_hbm.at[pl.ds(k_start, kslice), :], kslice_ref, sems.at[11]))
    copies[11].start()
    feats_ref, pos_ref = held[0], held[1]
    for copy in copies[:6]:
        copy.wait()
    pos = position_tile(pos_ref)
    out_ref[:, 4, :, :] = jnp.broadcast_to(feats_ref[:, :LANES][None], (SLICES, ROWS, LANES))
    for index, tile in enumerate(edge_tiles(count_ref, *held[2:6])):
        out_ref[:, 5 + index, :, :] = jnp.broadcast_to(tile.astype(BF16)[None], (SLICES, ROWS, LANES))
    x = feats_ref[...].astype(F32)
    for order in range(5):
        copies[6 + order].wait()
        weight = held[6 + order]
        offset, blocks = SPANS[order]
        start, width = offset * LANES, blocks * LANES
        if order == 0:
            conv_ref[:, :width] = jnp.dot(x[:, :width].astype(BF16), weight[...], preferred_element_type=F32)
            continue
        stacked = jnp.concatenate([x[:, start : start + width], x[:, start + width : start + 2 * width]], axis=0)
        lead, trail = pair_product(stacked.astype(BF16), weight)
        conv_ref[:, start : start + width] = lead
        conv_ref[:, start + width : start + 2 * width] = trail
    place = lax.broadcasted_iota(jnp.int32, (ROWS, LANES), 1) // CH
    for tile_index in range(4):
        for piece in range(SLICES):
            tile = pos if tile_index == 3 else jnp.zeros((ROWS, LANES), F32)
            for within in range(min(8, BLOCKS - 8 * tile_index)):
                block = 8 * tile_index + within
                moved = conv_ref[:, block * LANES : (block + 1) * LANES]
                if within != piece:
                    moved = pltpu.roll(moved, (CH * (within - piece)) % LANES, 1)
                tile = jnp.where(place == within, moved * math.sqrt(0.5), tile)
            out_ref[piece, tile_index, :, :] = tile.astype(BF16)
    copies[11].wait()


def spread_kernel(parts_ref, out_hbm, pos_ref, sems):
    copies = [
        pltpu.make_async_copy(parts_ref.at[:, pl.ds(0, 5)], out_hbm.at[index], sems.at[index]) for index in range(TGT)
    ]
    for copy in copies:
        copy.start()
    pos_ref[...] = parts_ref[:, 3, :, :]
    for copy in copies:
        copy.wait()


def main_kernel(
    count_ref,
    feats_hbm,
    group_ref,
    pos_ref0,
    pos_ref1,
    pos_ref2,
    pos_ref3,
    kidx_ref,
    *refs,
):
    kfilter_ref, out_ref = refs[:2]
    feats_ref, src_ref, tgt_ref, coef_ref, xt_ref, rows_ref, yt_ref, acc_ref, list_ref, sems = refs[2:]
    zone = lax.axis_index("zh")
    piece = lax.axis_index("y") * R + lax.axis_index("r")
    target_group = lax.axis_index("tgt")
    kslice = SRC * ROWS
    k_start = pl.multiple_of(piece * kslice, kslice)
    feats_copy = pltpu.make_async_copy(feats_hbm, feats_ref, sems.at[0])
    feats_copy.start()

    spare = pl.ds(ROWS * SLICES, ROWS)
    src_ref[spare, :] = jnp.zeros((ROWS, LANES), F32)
    tgt_ref[spare, :] = jnp.full((ROWS, LANES), SRC * ROWS, F32)
    for index in range(17):
        coef_ref[index, spare, :] = jnp.zeros((ROWS, LANES), F32)
    for tile in range(SLICES):
        rows = pl.ds(ROWS * tile, ROWS)
        src_ref[rows, :] = group_ref[tile, 5, :, :].astype(F32)
        tgt_ref[rows, :] = group_ref[tile, 6, :, :].astype(F32)
        angle = group_ref[tile, 7, :, :].astype(F32) + group_ref[tile, 8, :, :].astype(F32)
        scale = group_ref[tile, 9, :, :].astype(F32) * math.sqrt(0.5)
        c1, s1 = sincos_turns(angle * (0.5 / math.pi))
        c, s = c1, s1
        coef_ref[16, rows, :] = scale
        for order in range(4):
            if order:
                c, s = c * c1 - s * s1, s * c1 + c * s1
            coef_ref[4 * order, rows, :] = c
            coef_ref[4 * order + 1, rows, :] = s
            coef_ref[4 * order + 2, rows, :] = scale * c
            coef_ref[4 * order + 3, rows, :] = scale * s
    feats_copy.wait()
    for tile in range(SLICES):
        for index in range(4):
            block = feats_ref[:, tile, index, :, :].astype(F32).reshape(TGT * ROWS, LANES)
            width = min(LANES, COLS - index * LANES)
            xt_ref[tile, index * LANES : index * LANES + width, :] = block.T[:width].astype(BF16)

    per_step = STEP // LANES

    def list_tile(tile, at):
        source = (tile // R) * (ZH * R) + zone * R + tile % R
        steps = (count_ref[target_group, source] + STEP - 1) // STEP

        def put(step, place):
            list_ref[place] = tile * ROWS + step * per_step
            return place + 1

        return lax.fori_loop(0, steps, put, at)

    steps = lax.fori_loop(0, SLICES, list_tile, 0)
    list_ref[steps] = ROWS * SLICES

    acc_ref[...] = jnp.zeros_like(acc_ref)
    src_ids = lax.broadcasted_iota(jnp.int32, (TGT * ROWS, STEP), 0).astype(F32)
    tgt_ids = lax.broadcasted_iota(jnp.int32, (SRC * ROWS, 2 * STEP), 0).astype(F32)

    def two_steps(pair, carry):
        starts = [list_ref[2 * pair], list_ref[2 * pair + 1]]
        rows = [start + part for start in starts for part in range(per_step)]

        def lanes_of(rows, ref, *lead):
            return jnp.concatenate([ref[(*lead, pl.ds(row, 1), slice(None))] for row in rows], axis=1)

        for half in range(2):
            lanes = slice(half * STEP, (half + 1) * STEP)
            tile = jnp.minimum(starts[half] // ROWS, SLICES - 1)
            one_src = (src_ids == lanes_of(rows[half * per_step : (half + 1) * per_step], src_ref)).astype(F32)
            rows_ref[:, lanes] = jnp.dot(xt_ref[tile], one_src.astype(BF16), preferred_element_type=F32)
        width = SPANS[0][1] * CH
        scale = lanes_of(rows, coef_ref, 16)
        for low in range(0, width, CH):
            gathered = rows_ref[low : low + CH, :]
            yt_ref[low : low + CH, :] = ((gathered + gathered * lax.erf(gathered)) * scale).astype(BF16)
        for order in range(1, 5):
            offset, blocks = SPANS[order]
            cos_in, sin_in, cos_out, sin_out = (lanes_of(rows, coef_ref, 4 * (order - 1) + part) for part in range(4))
            for block in range(blocks):
                low = (offset + block) * CH
                high = low + blocks * CH
                lead, trail = rows_ref[low : low + CH, :], rows_ref[high : high + CH, :]
                lead, trail = cos_in * lead + sin_in * trail, cos_in * trail - sin_in * lead
                lead, trail = lead + lead * lax.erf(lead), trail + trail * lax.erf(trail)
                yt_ref[low : low + CH, :] = (cos_out * lead - sin_out * trail).astype(BF16)
                yt_ref[high : high + CH, :] = (cos_out * trail + sin_out * lead).astype(BF16)
        one_tgt = (tgt_ids == lanes_of(rows, tgt_ref)).astype(F32).astype(BF16)
        acc_ref[:, :COLS] += lax.dot_general(
            one_tgt, yt_ref[...], (((1,), (1,)), ((), ())), preferred_element_type=F32
        )
        return carry

    lax.fori_loop(0, (steps + 1) // 2, two_steps, 0)
    for index in range(4):
        out_ref[:, index, :, :] = (
            acc_ref[:, index * LANES : (index + 1) * LANES].reshape(SRC, ROWS, LANES).astype(BF16)
        )

    row_ids = lax.broadcasted_iota(jnp.int32, (LANES, kslice), 0)
    k_rows = kidx_ref[:, pl.ds(k_start, kslice)].astype(F32)
    k_table = jnp.zeros((LANES, kslice), F32)
    for axis in range(3):
        start = POS_LANE + 3 * axis
        k_table = jnp.where((row_ids >= start) & (row_ids < start + 3), k_rows[axis : axis + 1, :], k_table)
    atoms = SLICES * TGT * ROWS
    charges = feats_ref[:, :, 4, :, :].reshape(atoms, LANES)
    turns = lax.dot_general(
        k_table.T.astype(BF16),
        feats_ref[:, :, 3, :, :].reshape(atoms, LANES),
        (((1,), (1,)), ((), ())),
        preferred_element_type=F32,
    )
    own_pos = jnp.concatenate(
        [ref[...].reshape(SLICES * ROWS, LANES) for ref in (pos_ref0, pos_ref1, pos_ref2, pos_ref3)], axis=0
    )
    own_turns = jnp.dot(own_pos, k_table.astype(BF16), preferred_element_type=F32)
    total = jnp.zeros((kslice, LANES), F32)
    for table, own_table in zip(sincos_turns(turns), sincos_turns(own_turns)):
        factors = jnp.dot(table.astype(BF16), charges, preferred_element_type=F32)
        own_table = own_table.astype(BF16)
        for part in split2(kfilter_ref[...] * factors):
            total = total + jnp.dot(own_table, part, preferred_element_type=F32)
    for shift in range(ZH):
        from_zone = (zone + ZH - shift) % ZH
        for y in range(Y):
            low = (shift * SLICES + y * R) * ROWS
            out_ref[pl.ds(y * ZH * R + from_zone * R, R), 4, :, :] = (
                total[low : low + R * ROWS].reshape(R, ROWS, LANES).astype(BF16)
            )


def last_conv_kernel(norm, parts_ref, w0, w1, w2, w3, w4, update_ref, long_ref, conv_ref):
    total = jnp.zeros((ROWS, LANES), F32)
    for source in range(SRC):
        total = total + parts_ref[source, 4, :, :].astype(F32)
    long_ref[...] = total * norm
    place = lax.broadcasted_iota(jnp.int32, (ROWS, LANES), 1) // CH
    for index in range(4):
        sums = []
        for piece in range(SLICES):
            total = jnp.zeros((ROWS, LANES), F32)
            for zone in range(ZH):
                source = (piece // R) * (ZH * R) + zone * R + piece % R
                total = total + parts_ref[source, index, :, :].astype(F32)
            sums.append(total)
        for within in range(min(8, BLOCKS - 8 * index)):
            block = 8 * index + within
            tile = jnp.zeros((ROWS, LANES), F32)
            for piece in range(SLICES):
                moved = sums[piece]
                if within != piece:
                    moved = pltpu.roll(moved, (CH * (piece - within)) % LANES, 1)
                tile = jnp.where(place == piece, moved, tile)
            conv_ref[:, block * LANES : (block + 1) * LANES] = tile
    width = SPANS[0][1] * LANES
    value = conv_ref[:, :width]
    rounded = value.astype(BF16).astype(F32)
    stacked = jnp.concatenate([rounded, value - rounded], axis=0).astype(BF16)
    product = jnp.dot(stacked, w0[1], preferred_element_type=F32)
    update_ref[:, :width] = (product[:ROWS] + product[ROWS:]).astype(BF16)
    for order, weight in zip(range(1, 5), (w1, w2, w3, w4)):
        offset, blocks = SPANS[order]
        start, width = offset * LANES, blocks * LANES
        lead, trail = conv_ref[:, start : start + width], conv_ref[:, start + width : start + 2 * width]
        lead_high, trail_high = lead.astype(BF16).astype(F32), trail.astype(BF16).astype(F32)
        stacked = jnp.concatenate([lead_high, trail_high, lead - lead_high, trail - trail_high], axis=0)
        lead, trail = pair_product(stacked.astype(BF16), weight.at[1])
        update_ref[:, start : start + width] = lead.astype(BF16)
        update_ref[:, start + width : start + 2 * width] = trail.astype(BF16)


def params(mib):
    return pltpu.CompilerParams(vmem_limit_bytes=mib << 20)


def body(
    atom_feats,
    positions,
    edge_src,
    edge_tgt,
    edge_angle,
    edge_scale,
    edge_count,
    k_index,
    k_filter,
    *weights,
):
    slots = edge_src.shape[0]
    columns = atom_feats.shape[1]
    tile_shape = (ROWS, slots // ROWS)
    smem = pl.BlockSpec(memory_space=pltpu.SMEM)
    vmem = pl.BlockSpec(memory_space=pltpu.VMEM)
    hbm = pl.BlockSpec(memory_space=pltpu.HBM)
    counts = edge_count.T
    group_out = (SLICES, 10, ROWS, LANES)
    sources = (atom_feats, positions) + tuple(
        value.reshape(tile_shape) for value in (edge_src, edge_tgt, edge_angle, edge_scale)
    )
    kslice = SRC * ROWS
    group, k_filter = pl.pallas_call(
        first_kernel,
        out_shape=(jax.ShapeDtypeStruct(group_out, BF16), jax.ShapeDtypeStruct((kslice, LANES), F32)),
        in_specs=[smem] + [hbm] * 12,
        out_specs=(vmem, vmem),
        scratch_shapes=[pltpu.VMEM(value.shape, value.dtype) for value in sources]
        + [pltpu.VMEM(weight.shape[1:], weight.dtype) for weight in weights]
        + [pltpu.VMEM((ROWS, columns), F32), pltpu.SemaphoreType.DMA((12,))],
        compiler_params=params(56),
        cost_estimate=COST["first"],
        name="first",
    )(counts, *sources, *weights, k_filter)
    group = lax.all_to_all(group, ("y", "r"), 0, 0)
    feats_out = (TGT, SLICES, 5, ROWS, LANES)
    pos_out = (SLICES, ROWS, LANES)
    feats, pos = pl.pallas_call(
        spread_kernel,
        out_shape=(jax.ShapeDtypeStruct(feats_out, BF16), jax.ShapeDtypeStruct(pos_out, BF16)),
        in_specs=[vmem],
        out_specs=(hbm, vmem),
        scratch_shapes=[pltpu.SemaphoreType.DMA((TGT,))],
        compiler_params=params(32),
        cost_estimate=COST["spread"],
        name="spread",
    )(group)
    feats = lax.all_to_all(feats, "tgt", 0, 0)
    zones = [pos]
    for shift in range(1, ZH):
        zones.append(lax.ppermute(pos, "zh", [(i, (i + shift) % ZH) for i in range(ZH)]))

    parts_out = (SRC, 5, ROWS, LANES)
    parts = pl.pallas_call(
        main_kernel,
        out_shape=jax.ShapeDtypeStruct(parts_out, BF16),
        in_specs=[smem, hbm] + [vmem] * 7,
        out_specs=vmem,
        scratch_shapes=[
            pltpu.VMEM(feats_out, BF16),
            pltpu.VMEM(((SLICES + 1) * ROWS, LANES), F32),
            pltpu.VMEM(((SLICES + 1) * ROWS, LANES), F32),
            pltpu.VMEM((17, (SLICES + 1) * ROWS, LANES), F32),
            pltpu.VMEM((SLICES, COLS, TGT * ROWS), BF16),
            pltpu.VMEM((COLS, 2 * STEP), F32),
            pltpu.VMEM((COLS, 2 * STEP), BF16),
            pltpu.VMEM((kslice, 4 * LANES), F32),
            pltpu.SMEM((SLICES * (slots // STEP) + 1,), jnp.int32),
            pltpu.SemaphoreType.DMA((1,)),
        ],
        compiler_params=params(32),
        cost_estimate=COST["edge_sums"],
        name="edge_sums",
    )(counts, feats, group, *zones, k_index, k_filter)
    parts = lax.all_to_all(parts, SRC_AXES, 0, 0)

    norm = 1.0 / math.sqrt(SRC * TGT * ROWS * k_index.shape[1])
    return pl.pallas_call(
        lambda *refs: last_conv_kernel(norm, *refs),
        out_shape=(
            jax.ShapeDtypeStruct((ROWS, columns), BF16),
            jax.ShapeDtypeStruct((ROWS, LANES), F32),
        ),
        in_specs=[vmem] * 6,
        out_specs=(vmem, vmem),
        scratch_shapes=[pltpu.VMEM((ROWS, columns), F32)],
        compiler_params=params(16),
        cost_estimate=COST["last_conv"],
        name="last_conv",
    )(parts, *weights)


def solution(mesh):
    fine = Mesh(mesh.devices.reshape(Y, ZH, R, TGT), ALL_AXES)
    return jax.shard_map(
        body,
        mesh=fine,
        in_specs=(P(ALL_AXES, None), P(None, ALL_AXES)) + (P(ALL_AXES),) * 4 + (P(),) * 8,
        out_specs=(P(("tgt",) + SRC_AXES, None), P(ALL_AXES, None)),
        check_vma=False,
    )
```

```python
import math

import jax
import jax.numpy as jnp
from jax import lax
from jax.experimental import pallas as pl
from jax.experimental.pallas import tpu as pltpu
from jax.sharding import Mesh
from jax.sharding import PartitionSpec as P

Y, ZH, R, TGT = 2, 4, 4, 8
SRC_AXES = ("y", "zh", "r")
ALL_AXES = ("y", "zh", "r", "tgt")
SRC = Y * ZH * R
SLICES = Y * R
LANES = 128
ROWS = 8
BLOCKS = 25
CH = LANES // SLICES
COLS = BLOCKS * CH
HALF = 208
CUT = 256
STEP = 256
POS_LANE = 16
LAST_TILE, POS_TILE, CHARGE_TILE, TILES = 24, 25, 26, 34
COST = {
    "first": pl.CostEstimate(flops=50_000_000, transcendentals=0, bytes_accessed=3_000_000),
    "spread": pl.CostEstimate(flops=0, transcendentals=0, bytes_accessed=800_000),
    "edge_sums": pl.CostEstimate(flops=8_000_000_000, transcendentals=1_500_000, bytes_accessed=2_000_000),
    "message": pl.CostEstimate(flops=3_000_000_000, transcendentals=400_000, bytes_accessed=1_000_000),
    "last_conv": pl.CostEstimate(flops=100_000_000, transcendentals=0, bytes_accessed=3_200_000),
}
F32 = jnp.float32
BF16 = jnp.bfloat16


def order_spans():
    spans = [(0, 5)]
    offset = 5
    for order in range(1, 5):
        spans.append((offset, 5 - order))
        offset += 2 * (5 - order)
    return spans


SPANS = order_spans()


SIN_TERMS = (4.442867903, -7.307443419, 3.59478806, -0.7843739803)
COS_TERMS = (1.414213497, -6.978850988, 5.739461171, -1.88356299, 0.3106981923)


def series(terms, x2):
    value = terms[-1]
    for term in terms[-2::-1]:
        value = value * x2 + term
    return value


def sincos_turns(turns):
    part = turns - jnp.floor(turns + 0.5)
    x2 = part * part
    s = part * series(SIN_TERMS, x2)
    return 1.0 - s * s, s * series(COS_TERMS, x2)


def split2(value):
    high = value.astype(BF16)
    return high, (value - high.astype(F32)).astype(BF16)


def position_tile(pos_ref):
    row_ids = lax.broadcasted_iota(jnp.int32, (ROWS, ROWS), 0)
    col_ids = lax.broadcasted_iota(jnp.int32, (ROWS, ROWS), 1)
    lane = lax.broadcasted_iota(jnp.int32, (ROWS, LANES), 1)
    tile = jnp.zeros((ROWS, LANES), F32)
    for axis in range(3):
        spread = jnp.broadcast_to(pos_ref[axis : axis + 1, :], (ROWS, ROWS))
        rest = jnp.sum(jnp.where(row_ids == col_ids, spread, 0.0), axis=1, keepdims=True)
        for part in range(3):
            piece = rest.astype(BF16).astype(F32)
            rest = rest - piece
            tile = jnp.where(lane == POS_LANE + 3 * axis + part, piece, tile)
    return tile


def edge_tiles(count_ref, src_ref, tgt_ref, angle_ref, scale_ref):
    group = (lax.axis_index("y") * ZH + lax.axis_index("zh")) * R + lax.axis_index("r")
    count = count_ref[lax.axis_index("tgt"), group]
    slot = lax.broadcasted_iota(jnp.int32, (ROWS, LANES), 0) * LANES + lax.broadcasted_iota(
        jnp.int32, (ROWS, LANES), 1
    )
    angle = angle_ref[...]
    angle_high = angle.astype(BF16).astype(F32)
    return (
        src_ref[...].astype(F32),
        jnp.where(slot < count, tgt_ref[...], SRC * ROWS).astype(F32),
        angle_high,
        angle - angle_high,
        scale_ref[...],
    )


def pair_product(stacked, weight_ref):
    first = jnp.dot(stacked, weight_ref[0], preferred_element_type=F32)
    second = jnp.dot(stacked, weight_ref[1], preferred_element_type=F32)
    lead = jnp.zeros((ROWS, first.shape[1]), F32)
    trail = lead
    for base in range(0, stacked.shape[0], 2 * ROWS):
        lead = lead + (first[base : base + ROWS] - second[base + ROWS : base + 2 * ROWS])
        trail = trail + (second[base : base + ROWS] + first[base + ROWS : base + 2 * ROWS])
    return lead, trail


def first_kernel(count_ref, *refs):
    sources, kfilter_hbm, (out_ref, kslice_ref) = refs[:11], refs[11], refs[12:14]
    held, (conv_ref, sems) = refs[14:25], refs[25:]
    copies = [
        pltpu.make_async_copy(source if index < 6 else source.at[0], to, sems.at[index])
        for index, (source, to) in enumerate(zip(sources, held))
    ]
    for copy in copies:
        copy.start()
    kslice = kslice_ref.shape[0]
    k_start = pl.multiple_of((lax.axis_index("y") * R + lax.axis_index("r")) * kslice, kslice)
    copies.append(pltpu.make_async_copy(kfilter_hbm.at[pl.ds(k_start, kslice), :], kslice_ref, sems.at[11]))
    copies[11].start()
    feats_ref, pos_ref = held[0], held[1]
    for copy in copies[:6]:
        copy.wait()
    pos = position_tile(pos_ref)
    out_ref[:, 4, :, :] = jnp.broadcast_to(feats_ref[:, :LANES][None], (SLICES, ROWS, LANES))
    for index, tile in enumerate(edge_tiles(count_ref, *held[2:6])):
        out_ref[:, 5 + index, :, :] = jnp.broadcast_to(tile.astype(BF16)[None], (SLICES, ROWS, LANES))
    x = feats_ref[...].astype(F32)
    place = lax.broadcasted_iota(jnp.int32, (ROWS, LANES), 1) // CH

    def emit(tile_index):
        for piece in range(SLICES):
            tile = pos if tile_index == 3 else jnp.zeros((ROWS, LANES), F32)
            for within in range(min(8, BLOCKS - 8 * tile_index)):
                block = 8 * tile_index + within
                moved = conv_ref[:, block * LANES : (block + 1) * LANES]
                if within != piece:
                    moved = pltpu.roll(moved, (CH * (within - piece)) % LANES, 1)
                tile = jnp.where(place == within, moved, tile)
            out_ref[piece, tile_index, :, :] = tile.astype(BF16)

    root = math.sqrt(0.5)
    for order in range(5):
        copies[6 + order].wait()
        weight = held[6 + order]
        offset, blocks = SPANS[order]
        start, width = offset * LANES, blocks * LANES
        if order == 0:
            conv_ref[:, :width] = root * jnp.dot(x[:, :width].astype(BF16), weight[...], preferred_element_type=F32)
            continue
        stacked = jnp.concatenate([x[:, start : start + width], x[:, start + width : start + 2 * width]], axis=0)
        lead, trail = pair_product(stacked.astype(BF16), weight)
        conv_ref[:, start : start + width] = root * lead
        conv_ref[:, start + width : start + 2 * width] = root * trail
    for tile_index in range(4):
        emit(tile_index)
    copies[11].wait()


def group_lanes(tiles, first_lane):
    place = lax.broadcasted_iota(jnp.int32, (ROWS, LANES), 1) // CH
    packed = jnp.zeros((ROWS, LANES), F32)
    for index, tile in enumerate(tiles):
        shift = (CH * index - first_lane) % LANES
        packed = jnp.where(place == index, pltpu.roll(tile, shift, 1) if shift else tile, packed)
    return packed.astype(BF16)


def spread_kernel(parts_ref, out_hbm, pos_ref, held_ref, sems):
    mixed = [parts_ref[source, 3, :, :].astype(F32) for source in range(SLICES)]
    pos = group_lanes(mixed, POS_LANE)
    pos_ref[...] = pos
    for source in range(SLICES):
        held_ref[3 * source : 3 * source + 3, :, :] = parts_ref[source, :3, :, :]
        held_ref[CHARGE_TILE + source, :, :] = parts_ref[source, 4, :, :]
    held_ref[LAST_TILE, :, :] = group_lanes(mixed, 0)
    held_ref[POS_TILE, :, :] = pos
    copies = [pltpu.make_async_copy(held_ref, out_hbm.at[index], sems.at[index]) for index in range(TGT)]
    for copy in copies:
        copy.start()
    for copy in copies:
        copy.wait()


def main_kernel(
    count_ref,
    feats_hbm,
    group_ref,
    out_ref,
    feats_ref,
    src_ref,
    tgt_ref,
    coef_ref,
    xt_ref,
    rows_ref,
    yt_ref,
    acc_ref,
    list_ref,
    sems,
):
    zone = lax.axis_index("zh")
    target_group = lax.axis_index("tgt")
    feats_copy = pltpu.make_async_copy(feats_hbm, feats_ref, sems.at[0])
    feats_copy.start()

    spare = pl.ds(ROWS * SLICES, ROWS)
    src_ref[spare, :] = jnp.zeros((ROWS, LANES), F32)
    tgt_ref[spare, :] = jnp.full((ROWS, LANES), SRC * ROWS, F32)
    for index in range(17):
        coef_ref[index, spare, :] = jnp.zeros((ROWS, LANES), F32)
    for tile in range(SLICES):
        rows = pl.ds(ROWS * tile, ROWS)
        src_ref[rows, :] = group_ref[tile, 5, :, :].astype(F32)
        tgt_ref[rows, :] = group_ref[tile, 6, :, :].astype(F32)
        angle = group_ref[tile, 7, :, :].astype(F32) + group_ref[tile, 8, :, :].astype(F32)
        scale = group_ref[tile, 9, :, :].astype(F32) * math.sqrt(0.5)
        c1, s1 = sincos_turns(angle * (0.5 / math.pi))
        c, s = c1, s1
        coef_ref[16, rows, :] = scale
        for order in range(4):
            if order:
                c, s = c * c1 - s * s1, s * c1 + c * s1
            coef_ref[4 * order, rows, :] = c
            coef_ref[4 * order + 1, rows, :] = s
            coef_ref[4 * order + 2, rows, :] = scale * c
            coef_ref[4 * order + 3, rows, :] = scale * s
    feats_copy.wait()
    last = feats_ref[:, LAST_TILE, :, :].reshape(TGT * ROWS, LANES).T
    for tile in range(SLICES):
        for index in range(3):
            block = feats_ref[:, 3 * tile + index, :, :].reshape(TGT * ROWS, LANES)
            xt_ref[tile, index * LANES : (index + 1) * LANES, :] = block.T
        xt_ref[tile, 3 * LANES :, :] = last[tile * CH : (tile + 1) * CH]

    per_step = STEP // LANES

    def list_tile(tile, at):
        source = (tile // R) * (ZH * R) + zone * R + tile % R
        steps = (count_ref[target_group, source] + STEP - 1) // STEP

        def put(step, place):
            list_ref[place] = tile * ROWS + step * per_step
            return place + 1

        return lax.fori_loop(0, steps, put, at)

    for place in range(2):
        list_ref[place] = ROWS * SLICES
    end = lax.fori_loop(0, SLICES, list_tile, 2)
    for extra in range(3):
        list_ref[end + extra] = ROWS * SLICES
    pairs = (end - 1) // 2

    acc_ref[...] = jnp.zeros_like(acc_ref)
    yt_ref[...] = jnp.zeros_like(yt_ref)
    src_ids = lax.broadcasted_iota(jnp.int32, (TGT * ROWS, STEP), 0).astype(F32)
    tgt_ids = lax.broadcasted_iota(jnp.int32, (SRC * ROWS, 2 * STEP), 0).astype(F32)

    def lanes_of(rows, ref, *lead):
        return jnp.concatenate(
            [ref[(*lead, pl.ds(row + part, 1), slice(None))] for row in rows for part in range(per_step)], axis=1
        )

    def gather(rows, part):
        kept = slice(part * HALF, (part + 1) * HALF if part == 0 else COLS)
        for half, row in enumerate(rows):
            tile = jnp.minimum(row // ROWS, SLICES - 1)
            one_src = (src_ids == lanes_of([row], src_ref)).astype(F32).astype(BF16)
            rows_ref[kept, half * STEP : (half + 1) * STEP] = jnp.dot(
                xt_ref[tile, kept, :], one_src, preferred_element_type=F32
            )

    def convert(rows, order):
        offset, blocks = SPANS[order]
        if order == 0:
            scale = lanes_of(rows, coef_ref, 16)
            for low in range(0, blocks * CH, CH):
                gathered = rows_ref[low : low + CH, :]
                yt_ref[low : low + CH, :] = ((gathered + gathered * lax.erf(gathered)) * scale).astype(BF16)
            return
        cos_in, sin_in, cos_out, sin_out = (lanes_of(rows, coef_ref, 4 * (order - 1) + part) for part in range(4))
        for block in range(blocks):
            low = (offset + block) * CH
            high = low + blocks * CH
            lead, trail = rows_ref[low : low + CH, :], rows_ref[high : high + CH, :]
            lead, trail = cos_in * lead + sin_in * trail, cos_in * trail - sin_in * lead
            lead, trail = lead + lead * lax.erf(lead), trail + trail * lax.erf(trail)
            yt_ref[low : low + CH, :] = (cos_out * lead - sin_out * trail).astype(BF16)
            yt_ref[high : high + CH, :] = (cos_out * trail + sin_out * lead).astype(BF16)

    def scatter(rows, part):
        columns = slice(part * CUT, min((part + 1) * CUT, COLS))
        one_tgt = (tgt_ids == lanes_of(rows, tgt_ref)).astype(F32).astype(BF16)
        acc_ref[:, columns] += lax.dot_general(
            one_tgt, yt_ref[columns, :], (((1,), (1,)), ((), ())), preferred_element_type=F32
        )

    def two_rows(pair):
        return [list_ref[2 * pair], list_ref[2 * pair + 1]]

    def one_pair(pair, carry):
        before, now, then = (two_rows(pair + part) for part in range(3))
        scatter(before, 0)
        for order in (4, 3, 2):
            convert(now, order)
        gather(then, 1)
        scatter(now, 1)
        for order in (0, 1):
            convert(now, order)
        gather(then, 0)
        return carry

    for part in range(2):
        gather(two_rows(1), part)
    lax.fori_loop(0, pairs, one_pair, 0)
    scatter(two_rows(pairs), 0)
    for index in range(4):
        out_ref[:, index, :, :] = (
            acc_ref[:, index * LANES : (index + 1) * LANES].reshape(SRC, ROWS, LANES).astype(BF16)
        )


def spread_positions(packed):
    packed = packed.astype(F32)
    tiles = [packed] + [pltpu.roll(packed, LANES - CH * index, 1) for index in range(1, SLICES)]
    return jnp.concatenate(tiles, axis=0).astype(BF16)


def message_kernel(
    feats_ref, pos_ref0, pos_ref1, pos_ref2, pos_ref3, kidx_ref, kfilter_ref, parts_ref, out_ref
):
    del parts_ref
    zone = lax.axis_index("zh")
    piece = lax.axis_index("y") * R + lax.axis_index("r")
    kslice = SRC * ROWS
    k_start = pl.multiple_of(piece * kslice, kslice)
    row_ids = lax.broadcasted_iota(jnp.int32, (LANES, kslice), 0)
    k_rows = kidx_ref[:, pl.ds(k_start, kslice)].astype(F32)
    k_table = jnp.zeros((LANES, kslice), F32)
    for axis in range(3):
        k_table = jnp.where((row_ids >= 3 * axis) & (row_ids < 3 * axis + 3), k_rows[axis : axis + 1, :], k_table)
    charges = jnp.concatenate(
        [feats_ref[:, CHARGE_TILE + source, :, :].reshape(TGT * ROWS, LANES) for source in range(SLICES)], axis=0
    )
    turns = lax.dot_general(
        k_table.T.astype(BF16),
        spread_positions(feats_ref[:, POS_TILE, :, :].reshape(TGT * ROWS, LANES)),
        (((1,), (1,)), ((), ())),
        preferred_element_type=F32,
    )
    own_pos = jnp.concatenate(
        [spread_positions(ref[...]) for ref in (pos_ref0, pos_ref1, pos_ref2, pos_ref3)], axis=0
    )
    own_turns = jnp.dot(own_pos, k_table.astype(BF16), preferred_element_type=F32)
    total = jnp.zeros((kslice, LANES), F32)
    for table, own_table in zip(sincos_turns(turns), sincos_turns(own_turns)):
        factors = jnp.dot(table.astype(BF16), charges, preferred_element_type=F32)
        own_table = own_table.astype(BF16)
        for part in split2(kfilter_ref[...] * factors):
            total = total + jnp.dot(own_table, part, preferred_element_type=F32)
    for shift in range(ZH):
        from_zone = (zone + ZH - shift) % ZH
        for y in range(Y):
            low = (shift * SLICES + y * R) * ROWS
            out_ref[pl.ds(y * ZH * R + from_zone * R, R), 4, :, :] = (
                total[low : low + R * ROWS].reshape(R, ROWS, LANES).astype(BF16)
            )


def last_conv_kernel(norm, parts_ref, w0, w1, w2, w3, w4, update_ref, long_ref, conv_ref):
    total = jnp.zeros((ROWS, LANES), F32)
    for source in range(SRC):
        total = total + parts_ref[source, 4, :, :].astype(F32)
    long_ref[...] = total * norm
    place = lax.broadcasted_iota(jnp.int32, (ROWS, LANES), 1) // CH
    for index in range(4):
        sums = []
        for piece in range(SLICES):
            total = jnp.zeros((ROWS, LANES), F32)
            for zone in range(ZH):
                source = (piece // R) * (ZH * R) + zone * R + piece % R
                total = total + parts_ref[source, index, :, :].astype(F32)
            sums.append(total)
        for within in range(min(8, BLOCKS - 8 * index)):
            block = 8 * index + within
            tile = jnp.zeros((ROWS, LANES), F32)
            for piece in range(SLICES):
                moved = sums[piece]
                if within != piece:
                    moved = pltpu.roll(moved, (CH * (piece - within)) % LANES, 1)
                tile = jnp.where(place == piece, moved, tile)
            conv_ref[:, block * LANES : (block + 1) * LANES] = tile
    width = SPANS[0][1] * LANES
    value = conv_ref[:, :width]
    rounded = value.astype(BF16).astype(F32)
    stacked = jnp.concatenate([rounded, value - rounded], axis=0).astype(BF16)
    product = jnp.dot(stacked, w0[1], preferred_element_type=F32)
    update_ref[:, :width] = (product[:ROWS] + product[ROWS:]).astype(BF16)
    for order, weight in zip(range(1, 5), (w1, w2, w3, w4)):
        offset, blocks = SPANS[order]
        start, width = offset * LANES, blocks * LANES
        lead, trail = conv_ref[:, start : start + width], conv_ref[:, start + width : start + 2 * width]
        lead_high, trail_high = lead.astype(BF16).astype(F32), trail.astype(BF16).astype(F32)
        stacked = jnp.concatenate([lead_high, trail_high, lead - lead_high, trail - trail_high], axis=0)
        lead, trail = pair_product(stacked.astype(BF16), weight.at[1])
        update_ref[:, start : start + width] = lead.astype(BF16)
        update_ref[:, start + width : start + 2 * width] = trail.astype(BF16)


def params(mib):
    return pltpu.CompilerParams(vmem_limit_bytes=mib << 20)


def body(
    atom_feats,
    positions,
    edge_src,
    edge_tgt,
    edge_angle,
    edge_scale,
    edge_count,
    k_index,
    k_filter,
    *weights,
):
    slots = edge_src.shape[0]
    columns = atom_feats.shape[1]
    tile_shape = (ROWS, slots // ROWS)
    smem = pl.BlockSpec(memory_space=pltpu.SMEM)
    vmem = pl.BlockSpec(memory_space=pltpu.VMEM)
    hbm = pl.BlockSpec(memory_space=pltpu.HBM)
    counts = edge_count.T
    group_out = (SLICES, 10, ROWS, LANES)
    sources = (atom_feats, positions) + tuple(
        value.reshape(tile_shape) for value in (edge_src, edge_tgt, edge_angle, edge_scale)
    )
    kslice = SRC * ROWS
    group, k_filter = pl.pallas_call(
        first_kernel,
        out_shape=(jax.ShapeDtypeStruct(group_out, BF16), jax.ShapeDtypeStruct((kslice, LANES), F32)),
        in_specs=[smem] + [hbm] * 12,
        out_specs=(vmem, vmem),
        scratch_shapes=[pltpu.VMEM(value.shape, value.dtype) for value in sources]
        + [pltpu.VMEM(weight.shape[1:], weight.dtype) for weight in weights]
        + [pltpu.VMEM((ROWS, columns), F32), pltpu.SemaphoreType.DMA((12,))],
        compiler_params=params(56),
        cost_estimate=COST["first"],
        name="first",
    )(counts, *sources, *weights, k_filter)
    group = lax.all_to_all(group, ("y", "r"), 0, 0)
    feats_out = (TGT, TILES, ROWS, LANES)
    pos_out = (ROWS, LANES)
    feats, pos = pl.pallas_call(
        spread_kernel,
        out_shape=(jax.ShapeDtypeStruct(feats_out, BF16), jax.ShapeDtypeStruct(pos_out, BF16)),
        in_specs=[vmem],
        out_specs=(hbm, vmem),
        scratch_shapes=[pltpu.VMEM(feats_out[1:], BF16), pltpu.SemaphoreType.DMA((TGT,))],
        compiler_params=params(32),
        cost_estimate=COST["spread"],
        name="spread",
    )(group)
    feats = lax.all_to_all(feats, "tgt", 0, 0)
    zones = [pos]
    for shift in range(1, ZH):
        zones.append(lax.ppermute(pos, "zh", [(i, (i + shift) % ZH) for i in range(ZH)]))

    parts_out = (SRC, 5, ROWS, LANES)
    parts = pl.pallas_call(
        main_kernel,
        out_shape=jax.ShapeDtypeStruct(parts_out, BF16),
        in_specs=[smem, hbm, vmem],
        out_specs=vmem,
        scratch_shapes=[
            pltpu.VMEM(feats_out, BF16),
            pltpu.VMEM(((SLICES + 1) * ROWS, LANES), F32),
            pltpu.VMEM(((SLICES + 1) * ROWS, LANES), F32),
            pltpu.VMEM((17, (SLICES + 1) * ROWS, LANES), F32),
            pltpu.VMEM((SLICES, COLS, TGT * ROWS), BF16),
            pltpu.VMEM((COLS, 2 * STEP), F32),
            pltpu.VMEM((COLS, 2 * STEP), BF16),
            pltpu.VMEM((kslice, 4 * LANES), F32),
            pltpu.SMEM((SLICES * (slots // STEP) + 5,), jnp.int32),
            pltpu.SemaphoreType.DMA((1,)),
        ],
        compiler_params=params(32),
        cost_estimate=COST["edge_sums"],
        name="edge_sums",
    )(counts, feats, group)
    parts = pl.pallas_call(
        message_kernel,
        out_shape=jax.ShapeDtypeStruct(parts_out, BF16),
        in_specs=[vmem] * 8,
        out_specs=vmem,
        input_output_aliases={7: 0},
        compiler_params=params(32),
        cost_estimate=COST["message"],
        name="message",
    )(feats, *zones, k_index, k_filter, parts)
    parts = lax.all_to_all(parts, SRC_AXES, 0, 0)

    norm = 1.0 / math.sqrt(SRC * TGT * ROWS * k_index.shape[1])
    return pl.pallas_call(
        lambda *refs: last_conv_kernel(norm, *refs),
        out_shape=(
            jax.ShapeDtypeStruct((ROWS, columns), BF16),
            jax.ShapeDtypeStruct((ROWS, LANES), F32),
        ),
        in_specs=[vmem] * 6,
        out_specs=(vmem, vmem),
        scratch_shapes=[pltpu.VMEM((ROWS, columns), F32)],
        compiler_params=params(16),
        cost_estimate=COST["last_conv"],
        name="last_conv",
    )(parts, *weights)


def solution(mesh):
    fine = Mesh(mesh.devices.reshape(Y, ZH, R, TGT), ALL_AXES)
    return jax.shard_map(
        body,
        mesh=fine,
        in_specs=(P(ALL_AXES, None), P(None, ALL_AXES)) + (P(ALL_AXES),) * 4 + (P(),) * 8,
        out_specs=(P(("tgt",) + SRC_AXES, None), P(ALL_AXES, None)),
        check_vma=False,
    )
```

```python
import math

import jax
import jax.numpy as jnp
from jax import lax
from jax.experimental import pallas as pl
from jax.experimental.pallas import tpu as pltpu
from jax.sharding import Mesh
from jax.sharding import PartitionSpec as P

Y, ZH, R, TGT = 2, 4, 4, 8
SRC_AXES = ("y", "zh", "r")
ALL_AXES = ("y", "zh", "r", "tgt")
SRC = Y * ZH * R
SLICES = Y * R
LANES = 128
ROWS = 8
BLOCKS = 25
CH = LANES // SLICES
COLS = BLOCKS * CH
HALF = 208
CUT = 256
STEP = 256
POS_LANE = 16
MIX_LANE = 32
HALF_ROW = LANES // 2
K_SLICES = SLICES // 2
LAST_TILE, POS_TILE, CHARGE_TILE, TILES = 24, 25, 26, 30
COST = {
    "first": pl.CostEstimate(flops=50_000_000, transcendentals=0, bytes_accessed=3_000_000),
    "spread": pl.CostEstimate(flops=0, transcendentals=0, bytes_accessed=800_000),
    "edge_sums": pl.CostEstimate(flops=8_000_000_000, transcendentals=1_500_000, bytes_accessed=2_000_000),
    "message": pl.CostEstimate(flops=3_000_000_000, transcendentals=400_000, bytes_accessed=1_000_000),
    "last_conv": pl.CostEstimate(flops=100_000_000, transcendentals=0, bytes_accessed=3_200_000),
}
F32 = jnp.float32
BF16 = jnp.bfloat16


def order_spans():
    spans = [(0, 5)]
    offset = 5
    for order in range(1, 5):
        spans.append((offset, 5 - order))
        offset += 2 * (5 - order)
    return spans


SPANS = order_spans()


SIN_TERMS = (4.442867903, -7.307443419, 3.59478806, -0.7843739803)
COS_TERMS = (1.414213497, -6.978850988, 5.739461171, -1.88356299, 0.3106981923)


def series(terms, x2):
    value = terms[-1]
    for term in terms[-2::-1]:
        value = value * x2 + term
    return value


def sincos_turns(turns):
    part = turns - jnp.round(turns)
    x2 = part * part
    s = part * series(SIN_TERMS, x2)
    return 1.0 - s * s, s * series(COS_TERMS, x2)


def split2(value):
    high = value.astype(BF16)
    return high, (value - high.astype(F32)).astype(BF16)


def position_tile(pos_ref):
    row_ids = lax.broadcasted_iota(jnp.int32, (ROWS, ROWS), 0)
    col_ids = lax.broadcasted_iota(jnp.int32, (ROWS, ROWS), 1)
    lane = lax.broadcasted_iota(jnp.int32, (ROWS, LANES), 1)
    tile = jnp.zeros((ROWS, LANES), F32)
    for axis in range(3):
        spread = jnp.broadcast_to(pos_ref[axis : axis + 1, :], (ROWS, ROWS))
        rest = jnp.sum(jnp.where(row_ids == col_ids, spread, 0.0), axis=1, keepdims=True)
        for part in range(3):
            piece = rest.astype(BF16).astype(F32)
            rest = rest - piece
            tile = jnp.where(lane == POS_LANE + 3 * axis + part, piece, tile)
    return tile


def edge_tiles(count_ref, src_ref, tgt_ref, angle_ref, scale_ref):
    group = (lax.axis_index("y") * ZH + lax.axis_index("zh")) * R + lax.axis_index("r")
    count = count_ref[lax.axis_index("tgt"), group]
    slot = lax.broadcasted_iota(jnp.int32, (ROWS, LANES), 0) * LANES + lax.broadcasted_iota(
        jnp.int32, (ROWS, LANES), 1
    )
    angle = angle_ref[...]
    angle_high = angle.astype(BF16).astype(F32)
    return (
        src_ref[...].astype(F32),
        jnp.where(slot < count, tgt_ref[...], SRC * ROWS).astype(F32),
        angle_high,
        angle - angle_high,
        scale_ref[...],
    )


def pair_product(stacked, weight_ref):
    first = jnp.dot(stacked, weight_ref[0], preferred_element_type=F32)
    second = jnp.dot(stacked, weight_ref[1], preferred_element_type=F32)
    lead = jnp.zeros((ROWS, first.shape[1]), F32)
    trail = lead
    for base in range(0, stacked.shape[0], 2 * ROWS):
        lead = lead + (first[base : base + ROWS] - second[base + ROWS : base + 2 * ROWS])
        trail = trail + (second[base : base + ROWS] + first[base + ROWS : base + 2 * ROWS])
    return lead, trail


def k_slice_index():
    return lax.axis_index("y") * (R // 2) + lax.axis_index("r") // 2


def in_mix(value):
    lane = lax.broadcasted_iota(jnp.int32, value.shape, value.ndim - 1)
    return jnp.where((lane >= MIX_LANE) & (lane < MIX_LANE + HALF_ROW), value, 0.0)


def first_kernel(count_ref, *refs):
    sources, kfilter_hbm, (out_ref, kslice_ref) = refs[:11], refs[11], refs[12:14]
    held, (conv_ref, sems) = refs[14:25], refs[25:]
    copies = [
        pltpu.make_async_copy(source if index < 6 else source.at[0], to, sems.at[index])
        for index, (source, to) in enumerate(zip(sources, held))
    ]
    for copy in copies:
        copy.start()
    kslice = kslice_ref.shape[0]
    k_start = pl.multiple_of(k_slice_index() * kslice, kslice)
    copies.append(pltpu.make_async_copy(kfilter_hbm.at[pl.ds(k_start, kslice), :], kslice_ref, sems.at[11]))
    copies[11].start()
    feats_ref, pos_ref = held[0], held[1]
    for copy in copies[:6]:
        copy.wait()
    pos = position_tile(pos_ref)
    for index, tile in enumerate(edge_tiles(count_ref, *held[2:6])):
        out_ref[:, 4 + index, :, :] = jnp.broadcast_to(tile.astype(BF16)[None], (SLICES, ROWS, LANES))
    x = feats_ref[...].astype(F32)
    mixed = [pos + in_mix(pltpu.roll(x[:, :LANES], (MIX_LANE - HALF_ROW * half) % LANES, 1)) for half in range(2)]
    place = lax.broadcasted_iota(jnp.int32, (ROWS, LANES), 1) // CH

    def emit(tile_index):
        for piece in range(SLICES):
            tile = mixed[piece % 2] if tile_index == 3 else jnp.zeros((ROWS, LANES), F32)
            for within in range(min(8, BLOCKS - 8 * tile_index)):
                block = 8 * tile_index + within
                moved = conv_ref[:, block * LANES : (block + 1) * LANES]
                if within != piece:
                    moved = pltpu.roll(moved, (CH * (within - piece)) % LANES, 1)
                tile = jnp.where(place == within, moved, tile)
            out_ref[piece, tile_index, :, :] = tile.astype(BF16)

    root = math.sqrt(0.5)
    for order in range(5):
        copies[6 + order].wait()
        weight = held[6 + order]
        offset, blocks = SPANS[order]
        start, width = offset * LANES, blocks * LANES
        if order == 0:
            conv_ref[:, :width] = root * jnp.dot(x[:, :width].astype(BF16), weight[...], preferred_element_type=F32)
            continue
        stacked = jnp.concatenate([x[:, start : start + width], x[:, start + width : start + 2 * width]], axis=0)
        lead, trail = pair_product(stacked.astype(BF16), weight)
        conv_ref[:, start : start + width] = root * lead
        conv_ref[:, start + width : start + 2 * width] = root * trail
    for tile_index in range(4):
        emit(tile_index)
    copies[11].wait()


def group_lanes(tiles, first_lane):
    place = lax.broadcasted_iota(jnp.int32, (ROWS, LANES), 1) // CH
    packed = jnp.zeros((ROWS, LANES), F32)
    for index, tile in enumerate(tiles):
        shift = (CH * index - first_lane) % LANES
        packed = jnp.where(place == index, pltpu.roll(tile, shift, 1) if shift else tile, packed)
    return packed.astype(BF16)


def spread_kernel(parts_ref, out_hbm, pos_ref, held_ref, sems):
    mixed = [parts_ref[source, 3, :, :].astype(F32) for source in range(SLICES)]
    pos = group_lanes(mixed, POS_LANE)
    pos_ref[...] = pos
    for source in range(SLICES):
        held_ref[3 * source : 3 * source + 3, :, :] = parts_ref[source, :3, :, :]
    lane = lax.broadcasted_iota(jnp.int32, (ROWS, LANES), 1)
    for pair in range(SLICES // 2):
        left = pltpu.roll(mixed[2 * pair], LANES - MIX_LANE, 1)
        right = pltpu.roll(mixed[2 * pair + 1], HALF_ROW - MIX_LANE, 1)
        held_ref[CHARGE_TILE + pair, :, :] = jnp.where(lane < HALF_ROW, left, right).astype(BF16)
    held_ref[LAST_TILE, :, :] = group_lanes(mixed, 0)
    held_ref[POS_TILE, :, :] = pos
    copies = [pltpu.make_async_copy(held_ref, out_hbm.at[index], sems.at[index]) for index in range(TGT)]
    for copy in copies:
        copy.start()
    for copy in copies:
        copy.wait()


def main_kernel(
    count_ref,
    feats_hbm,
    group_ref,
    out_ref,
    feats_ref,
    src_ref,
    tgt_ref,
    coef_ref,
    xt_ref,
    rows_ref,
    yt_ref,
    acc_ref,
    list_ref,
    sems,
):
    zone = lax.axis_index("zh")
    target_group = lax.axis_index("tgt")
    feats_copy = pltpu.make_async_copy(feats_hbm, feats_ref, sems.at[0])
    feats_copy.start()

    spare = pl.ds(ROWS * SLICES, ROWS)
    src_ref[spare, :] = jnp.zeros((ROWS, LANES), F32)
    tgt_ref[spare, :] = jnp.full((ROWS, LANES), SRC * ROWS, F32)
    for index in range(17):
        coef_ref[index, spare, :] = jnp.zeros((ROWS, LANES), F32)
    for tile in range(SLICES):
        rows = pl.ds(ROWS * tile, ROWS)
        src_ref[rows, :] = group_ref[tile, 4, :, :].astype(F32)
        tgt_ref[rows, :] = group_ref[tile, 5, :, :].astype(F32)
        angle = group_ref[tile, 6, :, :].astype(F32) + group_ref[tile, 7, :, :].astype(F32)
        scale = group_ref[tile, 8, :, :].astype(F32) * math.sqrt(0.5)
        c1, s1 = sincos_turns(angle * (0.5 / math.pi))
        c, s = c1, s1
        coef_ref[16, rows, :] = scale
        for order in range(4):
            if order:
                c, s = c * c1 - s * s1, s * c1 + c * s1
            coef_ref[4 * order, rows, :] = c
            coef_ref[4 * order + 1, rows, :] = s
            coef_ref[4 * order + 2, rows, :] = scale * c
            coef_ref[4 * order + 3, rows, :] = scale * s
    feats_copy.wait()
    last = feats_ref[:, LAST_TILE, :, :].reshape(TGT * ROWS, LANES).T
    for tile in range(SLICES):
        for index in range(3):
            block = feats_ref[:, 3 * tile + index, :, :].reshape(TGT * ROWS, LANES)
            xt_ref[tile, index * LANES : (index + 1) * LANES, :] = block.T
        xt_ref[tile, 3 * LANES :, :] = last[tile * CH : (tile + 1) * CH]

    per_step = STEP // LANES

    def list_tile(tile, at):
        source = (tile // R) * (ZH * R) + zone * R + tile % R
        steps = (count_ref[target_group, source] + STEP - 1) // STEP

        def put(step, place):
            list_ref[place] = tile * ROWS + step * per_step
            return place + 1

        return lax.fori_loop(0, steps, put, at)

    for place in range(2):
        list_ref[place] = ROWS * SLICES
    end = lax.fori_loop(0, SLICES, list_tile, 2)
    for extra in range(3):
        list_ref[end + extra] = ROWS * SLICES
    pairs = (end - 1) // 2

    acc_ref[...] = jnp.zeros_like(acc_ref)
    yt_ref[...] = jnp.zeros_like(yt_ref)
    src_ids = lax.broadcasted_iota(jnp.int32, (TGT * ROWS, STEP), 0).astype(F32)
    tgt_ids = lax.broadcasted_iota(jnp.int32, (SRC * ROWS, 2 * STEP), 0).astype(F32).astype(BF16)

    def lanes_of(rows, ref, *lead):
        return jnp.concatenate(
            [ref[(*lead, pl.ds(row + part, 1), slice(None))] for row in rows for part in range(per_step)], axis=1
        )

    def gather(rows, part):
        kept = slice(part * HALF, (part + 1) * HALF if part == 0 else COLS)
        for half, row in enumerate(rows):
            tile = jnp.minimum(row // ROWS, SLICES - 1)
            one_src = (src_ids == lanes_of([row], src_ref)).astype(F32).astype(BF16)
            rows_ref[kept, half * STEP : (half + 1) * STEP] = jnp.dot(
                xt_ref[tile, kept, :], one_src, preferred_element_type=F32
            )

    def convert(rows, order):
        offset, blocks = SPANS[order]
        if order == 0:
            scale = lanes_of(rows, coef_ref, 16)
            for low in range(0, blocks * CH, CH):
                gathered = rows_ref[low : low + CH, :]
                yt_ref[low : low + CH, :] = ((gathered + gathered * lax.erf(gathered)) * scale).astype(BF16)
            return
        cos_in, sin_in, cos_out, sin_out = (lanes_of(rows, coef_ref, 4 * (order - 1) + part) for part in range(4))
        for block in range(blocks):
            low = (offset + block) * CH
            high = low + blocks * CH
            lead, trail = rows_ref[low : low + CH, :], rows_ref[high : high + CH, :]
            lead, trail = cos_in * lead + sin_in * trail, cos_in * trail - sin_in * lead
            lead, trail = lead + lead * lax.erf(lead), trail + trail * lax.erf(trail)
            yt_ref[low : low + CH, :] = (cos_out * lead - sin_out * trail).astype(BF16)
            yt_ref[high : high + CH, :] = (cos_out * trail + sin_out * lead).astype(BF16)

    def scatter(rows, part):
        columns = slice(part * CUT, min((part + 1) * CUT, COLS))
        one_tgt = jnp.where(tgt_ids == lanes_of(rows, tgt_ref).astype(BF16), jnp.ones((), BF16), jnp.zeros((), BF16))
        acc_ref[:, columns] += lax.dot_general(
            one_tgt, yt_ref[columns, :], (((1,), (1,)), ((), ())), preferred_element_type=F32
        )

    def two_rows(pair):
        return [list_ref[2 * pair], list_ref[2 * pair + 1]]

    def one_pair(pair, carry):
        before, now, then = (two_rows(pair + part) for part in range(3))
        scatter(before, 0)
        for order in (4, 3, 2):
            convert(now, order)
        gather(then, 1)
        scatter(now, 1)
        for order in (0, 1):
            convert(now, order)
        gather(then, 0)
        return carry

    for part in range(2):
        gather(two_rows(1), part)
    lax.fori_loop(0, pairs, one_pair, 0)
    scatter(two_rows(pairs), 0)
    for index in range(4):
        out_ref[:, index, :, :] = (
            acc_ref[:, index * LANES : (index + 1) * LANES].reshape(SRC, ROWS, LANES).astype(BF16)
        )


EVEN_ODD = (*range(0, SLICES, 2), *range(1, SLICES, 2))


def spread_positions(packed, sources):
    packed = packed.astype(F32)
    tiles = [pltpu.roll(packed, LANES - CH * index, 1) if index else packed for index in sources]
    return jnp.concatenate(tiles, axis=0).astype(BF16)


def message_kernel(feats_ref, pos_ref0, pos_ref1, pos_ref2, pos_ref3, kidx_ref, kfilter_ref, parts_ref, out_ref):
    zone = lax.axis_index("zh")
    kslice = kfilter_ref.shape[0]
    k_start = pl.multiple_of(k_slice_index() * kslice, kslice)
    row_ids = lax.broadcasted_iota(jnp.int32, (LANES, kslice), 0)
    k_rows = kidx_ref[:, pl.ds(k_start, kslice)].astype(F32)
    k_table = jnp.zeros((LANES, kslice), F32)
    for axis in range(3):
        k_table = jnp.where((row_ids >= 3 * axis) & (row_ids < 3 * axis + 3), k_rows[axis : axis + 1, :], k_table)
    charges = jnp.concatenate(
        [feats_ref[:, CHARGE_TILE + pair, :, :].reshape(TGT * ROWS, LANES) for pair in range(SLICES // 2)], axis=0
    )
    atoms = charges.shape[0]
    turns = lax.dot_general(
        k_table.T.astype(BF16),
        spread_positions(feats_ref[:, POS_TILE, :, :].reshape(TGT * ROWS, LANES), EVEN_ODD),
        (((1,), (1,)), ((), ())),
        preferred_element_type=F32,
    )
    own_pos = jnp.concatenate(
        [spread_positions(ref[...], range(SLICES)) for ref in (pos_ref0, pos_ref1, pos_ref2, pos_ref3)], axis=0
    )
    own_turns = jnp.dot(own_pos, k_table.astype(BF16), preferred_element_type=F32)
    filters = kfilter_ref[...]
    filters = jnp.where(lax.axis_index("r") % 2 == 1, pltpu.roll(filters, HALF_ROW, 1), filters)
    total = jnp.zeros((SRC * ROWS, LANES), F32)
    for table, own_table in zip(sincos_turns(turns), sincos_turns(own_turns)):
        table = table.astype(BF16)
        even = jnp.dot(table[:, :atoms], charges, preferred_element_type=F32)
        odd = jnp.dot(table[:, atoms:], charges, preferred_element_type=F32)
        own_table = own_table.astype(BF16)
        for part in split2(filters * (even + pltpu.roll(odd, HALF_ROW, 1))):
            total = total + jnp.dot(own_table, part, preferred_element_type=F32)
    total = in_mix(pltpu.roll(total, MIX_LANE, 1))
    for shift in range(ZH):
        from_zone = (zone + ZH - shift) % ZH
        for y in range(Y):
            low = (shift * SLICES + y * R) * ROWS
            place = pl.ds(y * ZH * R + from_zone * R, R)
            out_ref[place, :3, :, :] = parts_ref[place, :3, :, :]
            out_ref[place, 3, :, :] = (
                parts_ref[place, 3, :, :].astype(F32) + total[low : low + R * ROWS].reshape(R, ROWS, LANES)
            ).astype(BF16)


def last_conv_kernel(norm, parts_ref, w0, w1, w2, w3, w4, update_ref, long_ref, conv_ref):
    halves = []
    for half in range(2):
        total = jnp.zeros((ROWS, LANES), F32)
        for source in range(half, SRC, 2):
            total = total + parts_ref[source, 3, :, :].astype(F32)
        halves.append(pltpu.roll(total, (HALF_ROW * half - MIX_LANE) % LANES, 1))
    lane = lax.broadcasted_iota(jnp.int32, (ROWS, LANES), 1)
    long_ref[...] = jnp.where(lane < HALF_ROW, *halves) * norm
    place = lax.broadcasted_iota(jnp.int32, (ROWS, LANES), 1) // CH
    for index in range(4):
        sums = []
        for piece in range(SLICES):
            total = jnp.zeros((ROWS, LANES), F32)
            for zone in range(ZH):
                source = (piece // R) * (ZH * R) + zone * R + piece % R
                total = total + parts_ref[source, index, :, :].astype(F32)
            sums.append(total)
        for within in range(min(8, BLOCKS - 8 * index)):
            block = 8 * index + within
            tile = jnp.zeros((ROWS, LANES), F32)
            for piece in range(SLICES):
                moved = sums[piece]
                if within != piece:
                    moved = pltpu.roll(moved, (CH * (piece - within)) % LANES, 1)
                tile = jnp.where(place == piece, moved, tile)
            conv_ref[:, block * LANES : (block + 1) * LANES] = tile
    width = SPANS[0][1] * LANES
    value = conv_ref[:, :width]
    rounded = value.astype(BF16).astype(F32)
    stacked = jnp.concatenate([rounded, value - rounded], axis=0).astype(BF16)
    product = jnp.dot(stacked, w0[1], preferred_element_type=F32)
    update_ref[:, :width] = (product[:ROWS] + product[ROWS:]).astype(BF16)
    for order, weight in zip(range(1, 5), (w1, w2, w3, w4)):
        offset, blocks = SPANS[order]
        start, width = offset * LANES, blocks * LANES
        lead, trail = conv_ref[:, start : start + width], conv_ref[:, start + width : start + 2 * width]
        lead_high, trail_high = lead.astype(BF16).astype(F32), trail.astype(BF16).astype(F32)
        stacked = jnp.concatenate([lead_high, trail_high, lead - lead_high, trail - trail_high], axis=0)
        lead, trail = pair_product(stacked.astype(BF16), weight.at[1])
        update_ref[:, start : start + width] = lead.astype(BF16)
        update_ref[:, start + width : start + 2 * width] = trail.astype(BF16)


def params(mib):
    return pltpu.CompilerParams(vmem_limit_bytes=mib << 20)


def body(
    atom_feats,
    positions,
    edge_src,
    edge_tgt,
    edge_angle,
    edge_scale,
    edge_count,
    k_index,
    k_filter,
    *weights,
):
    slots = edge_src.shape[0]
    columns = atom_feats.shape[1]
    tile_shape = (ROWS, slots // ROWS)
    smem = pl.BlockSpec(memory_space=pltpu.SMEM)
    vmem = pl.BlockSpec(memory_space=pltpu.VMEM)
    hbm = pl.BlockSpec(memory_space=pltpu.HBM)
    counts = edge_count.T
    group_out = (SLICES, 9, ROWS, LANES)
    sources = (atom_feats, positions) + tuple(
        value.reshape(tile_shape) for value in (edge_src, edge_tgt, edge_angle, edge_scale)
    )
    kslice = k_index.shape[1] // K_SLICES
    group, k_filter = pl.pallas_call(
        first_kernel,
        out_shape=(jax.ShapeDtypeStruct(group_out, BF16), jax.ShapeDtypeStruct((kslice, LANES), F32)),
        in_specs=[smem] + [hbm] * 12,
        out_specs=(vmem, vmem),
        scratch_shapes=[pltpu.VMEM(value.shape, value.dtype) for value in sources]
        + [pltpu.VMEM(weight.shape[1:], weight.dtype) for weight in weights]
        + [pltpu.VMEM((ROWS, columns), F32), pltpu.SemaphoreType.DMA((12,))],
        compiler_params=params(56),
        cost_estimate=COST["first"],
        name="first",
    )(counts, *sources, *weights, k_filter)
    group = lax.all_to_all(group, ("y", "r"), 0, 0)
    feats_out = (TGT, TILES, ROWS, LANES)
    pos_out = (ROWS, LANES)
    feats, pos = pl.pallas_call(
        spread_kernel,
        out_shape=(jax.ShapeDtypeStruct(feats_out, BF16), jax.ShapeDtypeStruct(pos_out, BF16)),
        in_specs=[vmem],
        out_specs=(hbm, vmem),
        scratch_shapes=[pltpu.VMEM(feats_out[1:], BF16), pltpu.SemaphoreType.DMA((TGT,))],
        compiler_params=params(32),
        cost_estimate=COST["spread"],
        name="spread",
    )(group)
    feats = lax.all_to_all(feats, "tgt", 0, 0)
    zones = [pos]
    for shift in range(1, ZH):
        zones.append(lax.ppermute(pos, "zh", [(i, (i + shift) % ZH) for i in range(ZH)]))

    parts_out = (SRC, 4, ROWS, LANES)
    parts = pl.pallas_call(
        main_kernel,
        out_shape=jax.ShapeDtypeStruct(parts_out, BF16),
        in_specs=[smem, hbm, vmem],
        out_specs=vmem,
        scratch_shapes=[
            pltpu.VMEM(feats_out, BF16),
            pltpu.VMEM(((SLICES + 1) * ROWS, LANES), F32),
            pltpu.VMEM(((SLICES + 1) * ROWS, LANES), F32),
            pltpu.VMEM((17, (SLICES + 1) * ROWS, LANES), F32),
            pltpu.VMEM((SLICES, COLS, TGT * ROWS), BF16),
            pltpu.VMEM((COLS, 2 * STEP), F32),
            pltpu.VMEM((COLS, 2 * STEP), BF16),
            pltpu.VMEM((SRC * ROWS, 4 * LANES), F32),
            pltpu.SMEM((SLICES * (slots // STEP) + 5,), jnp.int32),
            pltpu.SemaphoreType.DMA((1,)),
        ],
        compiler_params=params(32),
        cost_estimate=COST["edge_sums"],
        name="edge_sums",
    )(counts, feats, group)
    parts = pl.pallas_call(
        message_kernel,
        out_shape=jax.ShapeDtypeStruct(parts_out, BF16),
        in_specs=[vmem] * 8,
        out_specs=vmem,
        compiler_params=params(32),
        cost_estimate=COST["message"],
        name="message",
    )(feats, *zones, k_index, k_filter, parts)
    parts = lax.all_to_all(parts, SRC_AXES, 0, 0)

    norm = 1.0 / math.sqrt(SRC * TGT * ROWS * k_index.shape[1])
    return pl.pallas_call(
        lambda *refs: last_conv_kernel(norm, *refs),
        out_shape=(
            jax.ShapeDtypeStruct((ROWS, columns), BF16),
            jax.ShapeDtypeStruct((ROWS, LANES), F32),
        ),
        in_specs=[vmem] * 6,
        out_specs=(vmem, vmem),
        scratch_shapes=[pltpu.VMEM((ROWS, columns), F32)],
        compiler_params=params(16),
        cost_estimate=COST["last_conv"],
        name="last_conv",
    )(parts, *weights)


def solution(mesh):
    fine = Mesh(mesh.devices.reshape(Y, ZH, R, TGT), ALL_AXES)
    return jax.shard_map(
        body,
        mesh=fine,
        in_specs=(P(ALL_AXES, None), P(None, ALL_AXES)) + (P(ALL_AXES),) * 4 + (P(),) * 8,
        out_specs=(P(("tgt",) + SRC_AXES, None), P(ALL_AXES, None)),
        check_vma=False,
    )
```

```python
import math

import jax
import jax.numpy as jnp
from jax import lax
from jax.experimental import pallas as pl
from jax.experimental.pallas import tpu as pltpu
from jax.sharding import Mesh
from jax.sharding import PartitionSpec as P

Y, ZH, R, TGT = 2, 4, 4, 8
SRC_AXES = ("y", "zh", "r")
ALL_AXES = ("y", "zh", "r", "tgt")
SRC = Y * ZH * R
SLICES = Y * R
LANES = 128
ROWS = 8
BLOCKS = 25
CH = LANES // SLICES
COLS = BLOCKS * CH
HALF = 208
CUT = 256
STEP = 256
POS_LANE = 16
MIX_LANE = 32
HALF_ROW = LANES // 2
K_SLICES = SLICES // 2
LAST_TILE, POS_TILE, CHARGE_TILE, TILES = 24, 25, 26, 30
COST = {
    "first": pl.CostEstimate(flops=50_000_000, transcendentals=0, bytes_accessed=3_000_000),
    "spread": pl.CostEstimate(flops=0, transcendentals=0, bytes_accessed=800_000),
    "edge_sums": pl.CostEstimate(flops=8_000_000_000, transcendentals=1_500_000, bytes_accessed=2_000_000),
    "message": pl.CostEstimate(flops=3_000_000_000, transcendentals=400_000, bytes_accessed=1_000_000),
    "last_conv": pl.CostEstimate(flops=100_000_000, transcendentals=0, bytes_accessed=3_200_000),
}
F32 = jnp.float32
BF16 = jnp.bfloat16


def order_spans():
    spans = [(0, 5)]
    offset = 5
    for order in range(1, 5):
        spans.append((offset, 5 - order))
        offset += 2 * (5 - order)
    return spans


SPANS = order_spans()


SIN_TERMS = (4.442867903, -7.307443419, 3.59478806, -0.7843739803)
COS_TERMS = (1.414213497, -6.978850988, 5.739461171, -1.88356299, 0.3106981923)


def series(terms, x2):
    value = terms[-1]
    for term in terms[-2::-1]:
        value = value * x2 + term
    return value


def sincos_turns(turns):
    part = turns - jnp.round(turns)
    x2 = part * part
    s = part * series(SIN_TERMS, x2)
    return 1.0 - s * s, s * series(COS_TERMS, x2)


def split2(value):
    high = value.astype(BF16)
    return high, (value - high.astype(F32)).astype(BF16)


def position_tile(pos_ref):
    row_ids = lax.broadcasted_iota(jnp.int32, (ROWS, ROWS), 0)
    col_ids = lax.broadcasted_iota(jnp.int32, (ROWS, ROWS), 1)
    lane = lax.broadcasted_iota(jnp.int32, (ROWS, LANES), 1)
    tile = jnp.zeros((ROWS, LANES), F32)
    for axis in range(3):
        spread = jnp.broadcast_to(pos_ref[axis : axis + 1, :], (ROWS, ROWS))
        rest = jnp.sum(jnp.where(row_ids == col_ids, spread, 0.0), axis=1, keepdims=True)
        for part in range(3):
            piece = rest.astype(BF16).astype(F32)
            rest = rest - piece
            tile = jnp.where(lane == POS_LANE + 3 * axis + part, piece, tile)
    return tile


def edge_tiles(count_ref, src_ref, tgt_ref, angle_ref, scale_ref):
    group = (lax.axis_index("y") * ZH + lax.axis_index("zh")) * R + lax.axis_index("r")
    count = count_ref[lax.axis_index("tgt"), group]
    slot = lax.broadcasted_iota(jnp.int32, (ROWS, LANES), 0) * LANES + lax.broadcasted_iota(
        jnp.int32, (ROWS, LANES), 1
    )
    angle = angle_ref[...]
    angle_high = angle.astype(BF16).astype(F32)
    return (
        src_ref[...].astype(F32),
        jnp.where(slot < count, tgt_ref[...], SRC * ROWS).astype(F32),
        angle_high,
        angle - angle_high,
        scale_ref[...],
    )


def pair_product(stacked, weight_ref):
    first = jnp.dot(stacked, weight_ref[0], preferred_element_type=F32)
    second = jnp.dot(stacked, weight_ref[1], preferred_element_type=F32)
    lead = jnp.zeros((ROWS, first.shape[1]), F32)
    trail = lead
    for base in range(0, stacked.shape[0], 2 * ROWS):
        lead = lead + (first[base : base + ROWS] - second[base + ROWS : base + 2 * ROWS])
        trail = trail + (second[base : base + ROWS] + first[base + ROWS : base + 2 * ROWS])
    return lead, trail


def k_slice_index():
    return lax.axis_index("y") * (R // 2) + lax.axis_index("r") // 2


def in_mix(value):
    lane = lax.broadcasted_iota(jnp.int32, value.shape, value.ndim - 1)
    return jnp.where((lane >= MIX_LANE) & (lane < MIX_LANE + HALF_ROW), value, 0.0)


def first_kernel(count_hbm, *refs):
    sources, out_ref, held, (conv_ref, count_ref, sems) = refs[:11], refs[11], refs[12:23], refs[23:]
    copies = [
        pltpu.make_async_copy(source if index < 6 else source.at[0], to, sems.at[index])
        for index, (source, to) in enumerate(zip(sources, held))
    ]
    count_copy = pltpu.make_async_copy(count_hbm, count_ref, sems.at[11])
    count_copy.start()
    for copy in copies:
        copy.start()
    feats_ref, pos_ref = held[0], held[1]
    for copy in copies[:6]:
        copy.wait()
    pos = position_tile(pos_ref)
    count_copy.wait()
    for index, tile in enumerate(edge_tiles(count_ref, *held[2:6])):
        out_ref[:, 4 + index, :, :] = jnp.broadcast_to(tile.astype(BF16)[None], (SLICES, ROWS, LANES))
    x = feats_ref[...].astype(F32)
    mixed = [pos + in_mix(pltpu.roll(x[:, :LANES], (MIX_LANE - HALF_ROW * half) % LANES, 1)) for half in range(2)]
    place = lax.broadcasted_iota(jnp.int32, (ROWS, LANES), 1) // CH

    def emit(tile_index):
        for piece in range(SLICES):
            tile = mixed[piece % 2] if tile_index == 3 else jnp.zeros((ROWS, LANES), F32)
            for within in range(min(8, BLOCKS - 8 * tile_index)):
                block = 8 * tile_index + within
                moved = conv_ref[:, block * LANES : (block + 1) * LANES]
                if within != piece:
                    moved = pltpu.roll(moved, (CH * (within - piece)) % LANES, 1)
                tile = jnp.where(place == within, moved, tile)
            out_ref[piece, tile_index, :, :] = tile.astype(BF16)

    root = math.sqrt(0.5)
    for order in range(5):
        copies[6 + order].wait()
        weight = held[6 + order]
        offset, blocks = SPANS[order]
        start, width = offset * LANES, blocks * LANES
        if order == 0:
            conv_ref[:, :width] = root * jnp.dot(x[:, :width].astype(BF16), weight[...], preferred_element_type=F32)
            continue
        stacked = jnp.concatenate([x[:, start : start + width], x[:, start + width : start + 2 * width]], axis=0)
        lead, trail = pair_product(stacked.astype(BF16), weight)
        conv_ref[:, start : start + width] = root * lead
        conv_ref[:, start + width : start + 2 * width] = root * trail
    for tile_index in range(4):
        emit(tile_index)


def group_lanes(tiles, first_lane):
    place = lax.broadcasted_iota(jnp.int32, (ROWS, LANES), 1) // CH
    packed = jnp.zeros((ROWS, LANES), F32)
    for index, tile in enumerate(tiles):
        shift = (CH * index - first_lane) % LANES
        packed = jnp.where(place == index, pltpu.roll(tile, shift, 1) if shift else tile, packed)
    return packed.astype(BF16)


def spread_kernel(parts_ref, out_ref, pos_ref):
    def put(index, tile):
        out_ref[:, index, :, :] = jnp.broadcast_to(tile[None], (TGT, ROWS, LANES))

    mixed = [parts_ref[source, 3, :, :].astype(F32) for source in range(SLICES)]
    pos = group_lanes(mixed, POS_LANE)
    pos_ref[...] = pos
    for source in range(SLICES):
        for index in range(3):
            put(3 * source + index, parts_ref[source, index, :, :])
    lane = lax.broadcasted_iota(jnp.int32, (ROWS, LANES), 1)
    for pair in range(SLICES // 2):
        left = pltpu.roll(mixed[2 * pair], LANES - MIX_LANE, 1)
        right = pltpu.roll(mixed[2 * pair + 1], HALF_ROW - MIX_LANE, 1)
        put(CHARGE_TILE + pair, jnp.where(lane < HALF_ROW, left, right).astype(BF16))
    put(LAST_TILE, group_lanes(mixed, 0))
    put(POS_TILE, pos)


def main_kernel(
    count_hbm,
    feats_hbm,
    group_ref,
    out_ref,
    feats_ref,
    src_ref,
    tgt_ref,
    coef_ref,
    xt_ref,
    rows_ref,
    yt_ref,
    acc_ref,
    list_ref,
    count_ref,
    sems,
):
    zone = lax.axis_index("zh")
    target_group = lax.axis_index("tgt")
    feats_copy = pltpu.make_async_copy(feats_hbm, feats_ref, sems.at[0])
    feats_copy.start()
    count_copy = pltpu.make_async_copy(count_hbm, count_ref, sems.at[1])
    count_copy.start()

    spare = pl.ds(ROWS * SLICES, ROWS)
    src_ref[spare, :] = jnp.zeros((ROWS, LANES), F32)
    tgt_ref[spare, :] = jnp.full((ROWS, LANES), SRC * ROWS, F32)
    for index in range(17):
        coef_ref[index, spare, :] = jnp.zeros((ROWS, LANES), F32)
    for tile in range(SLICES):
        rows = pl.ds(ROWS * tile, ROWS)
        src_ref[rows, :] = group_ref[tile, 4, :, :].astype(F32)
        tgt_ref[rows, :] = group_ref[tile, 5, :, :].astype(F32)
        angle = group_ref[tile, 6, :, :].astype(F32) + group_ref[tile, 7, :, :].astype(F32)
        scale = group_ref[tile, 8, :, :].astype(F32) * math.sqrt(0.5)
        c1, s1 = sincos_turns(angle * (0.5 / math.pi))
        c, s = c1, s1
        coef_ref[16, rows, :] = scale
        for order in range(4):
            if order:
                c, s = c * c1 - s * s1, s * c1 + c * s1
            coef_ref[4 * order, rows, :] = c
            coef_ref[4 * order + 1, rows, :] = s
            coef_ref[4 * order + 2, rows, :] = scale * c
            coef_ref[4 * order + 3, rows, :] = scale * s
    feats_copy.wait()
    last = feats_ref[:, LAST_TILE, :, :].reshape(TGT * ROWS, LANES).T
    for tile in range(SLICES):
        for index in range(3):
            block = feats_ref[:, 3 * tile + index, :, :].reshape(TGT * ROWS, LANES)
            xt_ref[tile, index * LANES : (index + 1) * LANES, :] = block.T
        xt_ref[tile, 3 * LANES :, :] = last[tile * CH : (tile + 1) * CH]

    count_copy.wait()
    per_step = STEP // LANES

    def list_tile(tile, at):
        source = (tile // R) * (ZH * R) + zone * R + tile % R
        steps = (count_ref[target_group, source] + STEP - 1) // STEP

        def put(step, place):
            list_ref[place] = tile * ROWS + step * per_step
            return place + 1

        return lax.fori_loop(0, steps, put, at)

    for place in range(2):
        list_ref[place] = ROWS * SLICES
    end = lax.fori_loop(0, SLICES, list_tile, 2)
    for extra in range(3):
        list_ref[end + extra] = ROWS * SLICES
    pairs = (end - 1) // 2

    acc_ref[...] = jnp.zeros_like(acc_ref)
    yt_ref[...] = jnp.zeros_like(yt_ref)
    src_ids = lax.broadcasted_iota(jnp.int32, (TGT * ROWS, STEP), 0).astype(F32)
    tgt_ids = lax.broadcasted_iota(jnp.int32, (SRC * ROWS, 2 * STEP), 0).astype(F32).astype(BF16)

    def lanes_of(rows, ref, *lead):
        return jnp.concatenate(
            [ref[(*lead, pl.ds(row + part, 1), slice(None))] for row in rows for part in range(per_step)], axis=1
        )

    def gather(rows, part):
        kept = slice(part * HALF, (part + 1) * HALF if part == 0 else COLS)
        for half, row in enumerate(rows):
            tile = jnp.minimum(row // ROWS, SLICES - 1)
            one_src = (src_ids == lanes_of([row], src_ref)).astype(F32).astype(BF16)
            rows_ref[kept, half * STEP : (half + 1) * STEP] = jnp.dot(
                xt_ref[tile, kept, :], one_src, preferred_element_type=F32
            )

    def convert(rows, order):
        offset, blocks = SPANS[order]
        if order == 0:
            scale = lanes_of(rows, coef_ref, 16)
            for low in range(0, blocks * CH, CH):
                gathered = rows_ref[low : low + CH, :]
                yt_ref[low : low + CH, :] = ((gathered + gathered * lax.erf(gathered)) * scale).astype(BF16)
            return
        cos_in, sin_in, cos_out, sin_out = (lanes_of(rows, coef_ref, 4 * (order - 1) + part) for part in range(4))
        for block in range(blocks):
            low = (offset + block) * CH
            high = low + blocks * CH
            lead, trail = rows_ref[low : low + CH, :], rows_ref[high : high + CH, :]
            lead, trail = cos_in * lead + sin_in * trail, cos_in * trail - sin_in * lead
            lead, trail = lead + lead * lax.erf(lead), trail + trail * lax.erf(trail)
            yt_ref[low : low + CH, :] = (cos_out * lead - sin_out * trail).astype(BF16)
            yt_ref[high : high + CH, :] = (cos_out * trail + sin_out * lead).astype(BF16)

    def scatter(rows, part):
        columns = slice(part * CUT, min((part + 1) * CUT, COLS))
        one_tgt = jnp.where(tgt_ids == lanes_of(rows, tgt_ref).astype(BF16), jnp.ones((), BF16), jnp.zeros((), BF16))
        acc_ref[:, columns] += lax.dot_general(
            one_tgt, yt_ref[columns, :], (((1,), (1,)), ((), ())), preferred_element_type=F32
        )

    def two_rows(pair):
        return [list_ref[2 * pair], list_ref[2 * pair + 1]]

    def one_pair(pair, carry):
        before, now, then = (two_rows(pair + part) for part in range(3))
        scatter(before, 0)
        for order in (4, 3, 2):
            convert(now, order)
        gather(then, 1)
        scatter(now, 1)
        for order in (0, 1):
            convert(now, order)
        gather(then, 0)
        return carry

    for part in range(2):
        gather(two_rows(1), part)
    lax.fori_loop(0, pairs, one_pair, 0)
    scatter(two_rows(pairs), 0)
    for index in range(4):
        out_ref[:, index, :, :] = (
            acc_ref[:, index * LANES : (index + 1) * LANES].reshape(SRC, ROWS, LANES).astype(BF16)
        )


EVEN_ODD = (*range(0, SLICES, 2), *range(1, SLICES, 2))


def spread_positions(packed, sources):
    packed = packed.astype(F32)
    tiles = [pltpu.roll(packed, LANES - CH * index, 1) if index else packed for index in sources]
    return jnp.concatenate(tiles, axis=0).astype(BF16)


def message_kernel(feats_ref, pos_ref0, pos_ref1, pos_ref2, pos_ref3, kidx_ref, kfilter_ref, parts_ref, out_ref):
    zone = lax.axis_index("zh")
    kslice = kfilter_ref.shape[0] // K_SLICES
    k_start = pl.multiple_of(k_slice_index() * kslice, kslice)
    row_ids = lax.broadcasted_iota(jnp.int32, (LANES, kslice), 0)
    k_rows = kidx_ref[:, pl.ds(k_start, kslice)].astype(F32)
    k_table = jnp.zeros((LANES, kslice), F32)
    for axis in range(3):
        k_table = jnp.where((row_ids >= 3 * axis) & (row_ids < 3 * axis + 3), k_rows[axis : axis + 1, :], k_table)
    charges = jnp.concatenate(
        [feats_ref[:, CHARGE_TILE + pair, :, :].reshape(TGT * ROWS, LANES) for pair in range(SLICES // 2)], axis=0
    )
    atoms = charges.shape[0]
    turns = lax.dot_general(
        k_table.T.astype(BF16),
        spread_positions(feats_ref[:, POS_TILE, :, :].reshape(TGT * ROWS, LANES), EVEN_ODD),
        (((1,), (1,)), ((), ())),
        preferred_element_type=F32,
    )
    own_pos = jnp.concatenate(
        [spread_positions(ref[...], range(SLICES)) for ref in (pos_ref0, pos_ref1, pos_ref2, pos_ref3)], axis=0
    )
    own_turns = jnp.dot(own_pos, k_table.astype(BF16), preferred_element_type=F32)
    filters = kfilter_ref[pl.ds(k_start, kslice), :]
    filters = jnp.where(lax.axis_index("r") % 2 == 1, pltpu.roll(filters, HALF_ROW, 1), filters)
    total = jnp.zeros((SRC * ROWS, LANES), F32)
    for table, own_table in zip(sincos_turns(turns), sincos_turns(own_turns)):
        table = table.astype(BF16)
        even = jnp.dot(table[:, :atoms], charges, preferred_element_type=F32)
        odd = jnp.dot(table[:, atoms:], charges, preferred_element_type=F32)
        own_table = own_table.astype(BF16)
        for part in split2(filters * (even + pltpu.roll(odd, HALF_ROW, 1))):
            total = total + jnp.dot(own_table, part, preferred_element_type=F32)
    total = in_mix(pltpu.roll(total, MIX_LANE, 1))
    for shift in range(ZH):
        from_zone = (zone + ZH - shift) % ZH
        for y in range(Y):
            low = (shift * SLICES + y * R) * ROWS
            place = pl.ds(y * ZH * R + from_zone * R, R)
            out_ref[place, :3, :, :] = parts_ref[place, :3, :, :]
            out_ref[place, 3, :, :] = (
                parts_ref[place, 3, :, :].astype(F32) + total[low : low + R * ROWS].reshape(R, ROWS, LANES)
            ).astype(BF16)


def last_conv_kernel(norm, parts_ref, w0, w1, w2, w3, w4, update_ref, long_ref, conv_ref):
    halves = []
    for half in range(2):
        total = jnp.zeros((ROWS, LANES), F32)
        for source in range(half, SRC, 2):
            total = total + parts_ref[source, 3, :, :].astype(F32)
        halves.append(pltpu.roll(total, (HALF_ROW * half - MIX_LANE) % LANES, 1))
    lane = lax.broadcasted_iota(jnp.int32, (ROWS, LANES), 1)
    long_ref[...] = jnp.where(lane < HALF_ROW, *halves) * norm
    place = lax.broadcasted_iota(jnp.int32, (ROWS, LANES), 1) // CH
    for index in range(4):
        sums = []
        for piece in range(SLICES):
            total = jnp.zeros((ROWS, LANES), F32)
            for zone in range(ZH):
                source = (piece // R) * (ZH * R) + zone * R + piece % R
                total = total + parts_ref[source, index, :, :].astype(F32)
            sums.append(total)
        for within in range(min(8, BLOCKS - 8 * index)):
            block = 8 * index + within
            tile = jnp.zeros((ROWS, LANES), F32)
            for piece in range(SLICES):
                moved = sums[piece]
                if within != piece:
                    moved = pltpu.roll(moved, (CH * (piece - within)) % LANES, 1)
                tile = jnp.where(place == piece, moved, tile)
            conv_ref[:, block * LANES : (block + 1) * LANES] = tile
    width = SPANS[0][1] * LANES
    value = conv_ref[:, :width]
    rounded = value.astype(BF16).astype(F32)
    stacked = jnp.concatenate([rounded, value - rounded], axis=0).astype(BF16)
    product = jnp.dot(stacked, w0[1], preferred_element_type=F32)
    update_ref[:, :width] = (product[:ROWS] + product[ROWS:]).astype(BF16)
    for order, weight in zip(range(1, 5), (w1, w2, w3, w4)):
        offset, blocks = SPANS[order]
        start, width = offset * LANES, blocks * LANES
        lead, trail = conv_ref[:, start : start + width], conv_ref[:, start + width : start + 2 * width]
        lead_high, trail_high = lead.astype(BF16).astype(F32), trail.astype(BF16).astype(F32)
        stacked = jnp.concatenate([lead_high, trail_high, lead - lead_high, trail - trail_high], axis=0)
        lead, trail = pair_product(stacked.astype(BF16), weight.at[1])
        update_ref[:, start : start + width] = lead.astype(BF16)
        update_ref[:, start + width : start + 2 * width] = trail.astype(BF16)


def params(mib):
    return pltpu.CompilerParams(vmem_limit_bytes=mib << 20)


def body(
    atom_feats,
    positions,
    edge_src,
    edge_tgt,
    edge_angle,
    edge_scale,
    edge_count,
    k_index,
    k_filter,
    *weights,
):
    slots = edge_src.shape[0]
    columns = atom_feats.shape[1]
    tile_shape = (ROWS, slots // ROWS)
    vmem = pl.BlockSpec(memory_space=pltpu.VMEM)
    hbm = pl.BlockSpec(memory_space=pltpu.HBM)
    counts = edge_count.T
    group_out = (SLICES, 9, ROWS, LANES)
    sources = (atom_feats, positions) + tuple(
        value.reshape(tile_shape) for value in (edge_src, edge_tgt, edge_angle, edge_scale)
    )
    group = pl.pallas_call(
        first_kernel,
        out_shape=jax.ShapeDtypeStruct(group_out, BF16),
        in_specs=[hbm] * 12,
        out_specs=vmem,
        scratch_shapes=[pltpu.VMEM(value.shape, value.dtype) for value in sources]
        + [pltpu.VMEM(weight.shape[1:], weight.dtype) for weight in weights]
        + [pltpu.VMEM((ROWS, columns), F32), pltpu.SMEM(counts.shape, jnp.int32), pltpu.SemaphoreType.DMA((12,))],
        compiler_params=params(56),
        cost_estimate=COST["first"],
        name="first",
    )(counts, *sources, *weights)
    group = lax.all_to_all(group, ("y", "r"), 0, 0)
    feats_out = (TGT, TILES, ROWS, LANES)
    pos_out = (ROWS, LANES)
    feats, pos = pl.pallas_call(
        spread_kernel,
        out_shape=(jax.ShapeDtypeStruct(feats_out, BF16), jax.ShapeDtypeStruct(pos_out, BF16)),
        in_specs=[vmem],
        out_specs=(vmem, vmem),
        compiler_params=params(32),
        cost_estimate=COST["spread"],
        name="spread",
    )(group)
    feats = lax.all_to_all(feats, "tgt", 0, 0)
    zones = [pos]
    for shift in range(1, ZH):
        zones.append(lax.ppermute(pos, "zh", [(i, (i + shift) % ZH) for i in range(ZH)]))

    parts_out = (SRC, 4, ROWS, LANES)
    parts = pl.pallas_call(
        main_kernel,
        out_shape=jax.ShapeDtypeStruct(parts_out, BF16),
        in_specs=[hbm, hbm, vmem],
        out_specs=vmem,
        scratch_shapes=[
            pltpu.VMEM(feats_out, BF16),
            pltpu.VMEM(((SLICES + 1) * ROWS, LANES), F32),
            pltpu.VMEM(((SLICES + 1) * ROWS, LANES), F32),
            pltpu.VMEM((17, (SLICES + 1) * ROWS, LANES), F32),
            pltpu.VMEM((SLICES, COLS, TGT * ROWS), BF16),
            pltpu.VMEM((COLS, 2 * STEP), F32),
            pltpu.VMEM((COLS, 2 * STEP), BF16),
            pltpu.VMEM((SRC * ROWS, 4 * LANES), F32),
            pltpu.SMEM((SLICES * (slots // STEP) + 5,), jnp.int32),
            pltpu.SMEM(counts.shape, jnp.int32),
            pltpu.SemaphoreType.DMA((2,)),
        ],
        compiler_params=params(32),
        cost_estimate=COST["edge_sums"],
        name="edge_sums",
    )(counts, feats, group)
    parts = pl.pallas_call(
        message_kernel,
        out_shape=jax.ShapeDtypeStruct(parts_out, BF16),
        in_specs=[vmem] * 8,
        out_specs=vmem,
        compiler_params=params(32),
        cost_estimate=COST["message"],
        name="message",
    )(feats, *zones, k_index, k_filter, parts)
    parts = lax.all_to_all(parts, SRC_AXES, 0, 0)

    norm = 1.0 / math.sqrt(SRC * TGT * ROWS * k_index.shape[1])
    return pl.pallas_call(
        lambda *refs: last_conv_kernel(norm, *refs),
        out_shape=(
            jax.ShapeDtypeStruct((ROWS, columns), BF16),
            jax.ShapeDtypeStruct((ROWS, LANES), F32),
        ),
        in_specs=[vmem] * 6,
        out_specs=(vmem, vmem),
        scratch_shapes=[pltpu.VMEM((ROWS, columns), F32)],
        compiler_params=params(16),
        cost_estimate=COST["last_conv"],
        name="last_conv",
    )(parts, *weights)


def solution(mesh):
    fine = Mesh(mesh.devices.reshape(Y, ZH, R, TGT), ALL_AXES)
    return jax.shard_map(
        body,
        mesh=fine,
        in_specs=(P(ALL_AXES, None), P(None, ALL_AXES)) + (P(ALL_AXES),) * 4 + (P(),) * 8,
        out_specs=(P(("tgt",) + SRC_AXES, None), P(ALL_AXES, None)),
        check_vma=False,
    )
```

```python
import math

import jax
import jax.numpy as jnp
from jax import lax
from jax.experimental import pallas as pl
from jax.experimental.pallas import tpu as pltpu
from jax.sharding import Mesh
from jax.sharding import PartitionSpec as P

Y, ZH, R, TGT = 2, 4, 4, 8
SRC_AXES = ("y", "zh", "r")
ALL_AXES = ("y", "zh", "r", "tgt")
SRC = Y * ZH * R
SLICES = Y * R
LANES = 128
ROWS = 8
BLOCKS = 25
CH = LANES // SLICES
COLS = BLOCKS * CH
HALF = 208
CUT = 256
STEP = 256
POS_LANE = 16
MIX_LANE = 32
HALF_ROW = LANES // 2
K_SLICES = SLICES // 2
LAST_TILE, POS_TILE, CHARGE_TILE, TILES = 24, 25, 26, 30
COST = {
    "first": pl.CostEstimate(flops=50_000_000, transcendentals=0, bytes_accessed=3_000_000),
    "spread": pl.CostEstimate(flops=0, transcendentals=0, bytes_accessed=800_000),
    "edge_sums": pl.CostEstimate(flops=8_000_000_000, transcendentals=1_500_000, bytes_accessed=2_000_000),
    "message": pl.CostEstimate(flops=3_000_000_000, transcendentals=400_000, bytes_accessed=1_000_000),
    "last_conv": pl.CostEstimate(flops=100_000_000, transcendentals=0, bytes_accessed=3_200_000),
}
F32 = jnp.float32
BF16 = jnp.bfloat16


def order_spans():
    spans = [(0, 5)]
    offset = 5
    for order in range(1, 5):
        spans.append((offset, 5 - order))
        offset += 2 * (5 - order)
    return spans


SPANS = order_spans()


SIN_TERMS = (4.442867903, -7.307443419, 3.59478806, -0.7843739803)
COS_TERMS = (1.414213497, -6.978850988, 5.739461171, -1.88356299, 0.3106981923)


def series(terms, x2):
    value = terms[-1]
    for term in terms[-2::-1]:
        value = value * x2 + term
    return value


def sincos_turns(turns):
    part = turns - jnp.round(turns)
    x2 = part * part
    s = part * series(SIN_TERMS, x2)
    return 1.0 - s * s, s * series(COS_TERMS, x2)


def split2(value):
    high = value.astype(BF16)
    return high, (value - high.astype(F32)).astype(BF16)


def position_tile(pos_ref):
    row_ids = lax.broadcasted_iota(jnp.int32, (ROWS, ROWS), 0)
    col_ids = lax.broadcasted_iota(jnp.int32, (ROWS, ROWS), 1)
    lane = lax.broadcasted_iota(jnp.int32, (ROWS, LANES), 1)
    tile = jnp.zeros((ROWS, LANES), F32)
    for axis in range(3):
        spread = jnp.broadcast_to(pos_ref[axis : axis + 1, :], (ROWS, ROWS))
        rest = jnp.sum(jnp.where(row_ids == col_ids, spread, 0.0), axis=1, keepdims=True)
        for part in range(3):
            piece = rest.astype(BF16).astype(F32)
            rest = rest - piece
            tile = jnp.where(lane == POS_LANE + 3 * axis + part, piece, tile)
    return tile


def edge_tiles(count_ref, src_ref, tgt_ref, angle_ref, scale_ref):
    group = (lax.axis_index("y") * ZH + lax.axis_index("zh")) * R + lax.axis_index("r")
    count = count_ref[lax.axis_index("tgt"), group]
    slot = lax.broadcasted_iota(jnp.int32, (ROWS, LANES), 0) * LANES + lax.broadcasted_iota(
        jnp.int32, (ROWS, LANES), 1
    )
    angle = angle_ref[...]
    angle_high = angle.astype(BF16).astype(F32)
    return (
        src_ref[...].astype(F32),
        jnp.where(slot < count, tgt_ref[...], SRC * ROWS).astype(F32),
        angle_high,
        angle - angle_high,
        scale_ref[...],
    )


def pair_product(stacked, weight_ref):
    first = jnp.dot(stacked, weight_ref[0], preferred_element_type=F32)
    second = jnp.dot(stacked, weight_ref[1], preferred_element_type=F32)
    lead = jnp.zeros((ROWS, first.shape[1]), F32)
    trail = lead
    for base in range(0, stacked.shape[0], 2 * ROWS):
        lead = lead + (first[base : base + ROWS] - second[base + ROWS : base + 2 * ROWS])
        trail = trail + (second[base : base + ROWS] + first[base + ROWS : base + 2 * ROWS])
    return lead, trail


def k_slice_index():
    return lax.axis_index("y") * (R // 2) + lax.axis_index("r") // 2


def in_mix(value):
    lane = lax.broadcasted_iota(jnp.int32, value.shape, value.ndim - 1)
    return jnp.where((lane >= MIX_LANE) & (lane < MIX_LANE + HALF_ROW), value, 0.0)


def first_kernel(count_hbm, *refs):
    sources, out_ref, held, (conv_ref, count_ref, sems) = refs[:11], refs[11], refs[12:23], refs[23:]
    copies = [
        pltpu.make_async_copy(source if index < 6 else source.at[0], to, sems.at[index])
        for index, (source, to) in enumerate(zip(sources, held))
    ]
    count_copy = pltpu.make_async_copy(count_hbm, count_ref, sems.at[11])
    count_copy.start()
    for copy in copies:
        copy.start()
    feats_ref, pos_ref = held[0], held[1]
    for copy in copies[:6]:
        copy.wait()
    pos = position_tile(pos_ref)
    count_copy.wait()
    for index, tile in enumerate(edge_tiles(count_ref, *held[2:6])):
        out_ref[:, 4 + index, :, :] = jnp.broadcast_to(tile.astype(BF16)[None], (SLICES, ROWS, LANES))
    x = feats_ref[...].astype(F32)
    mixed = [pos + in_mix(pltpu.roll(x[:, :LANES], (MIX_LANE - HALF_ROW * half) % LANES, 1)) for half in range(2)]
    place = lax.broadcasted_iota(jnp.int32, (ROWS, LANES), 1) // CH

    def emit(tile_index):
        for piece in range(SLICES):
            tile = mixed[piece % 2] if tile_index == 3 else jnp.zeros((ROWS, LANES), F32)
            for within in range(min(8, BLOCKS - 8 * tile_index)):
                block = 8 * tile_index + within
                moved = conv_ref[:, block * LANES : (block + 1) * LANES]
                if within != piece:
                    moved = pltpu.roll(moved, (CH * (within - piece)) % LANES, 1)
                tile = jnp.where(place == within, moved, tile)
            out_ref[piece, tile_index, :, :] = tile.astype(BF16)

    root = math.sqrt(0.5)
    for order in range(5):
        copies[6 + order].wait()
        weight = held[6 + order]
        offset, blocks = SPANS[order]
        start, width = offset * LANES, blocks * LANES
        if order == 0:
            conv_ref[:, :width] = root * jnp.dot(x[:, :width].astype(BF16), weight[...], preferred_element_type=F32)
            continue
        stacked = jnp.concatenate([x[:, start : start + width], x[:, start + width : start + 2 * width]], axis=0)
        lead, trail = pair_product(stacked.astype(BF16), weight)
        conv_ref[:, start : start + width] = root * lead
        conv_ref[:, start + width : start + 2 * width] = root * trail
    for tile_index in range(4):
        emit(tile_index)


def group_lanes(tiles, first_lane):
    place = lax.broadcasted_iota(jnp.int32, (ROWS, LANES), 1) // CH
    packed = jnp.zeros((ROWS, LANES), F32)
    for index, tile in enumerate(tiles):
        shift = (CH * index - first_lane) % LANES
        packed = jnp.where(place == index, pltpu.roll(tile, shift, 1) if shift else tile, packed)
    return packed.astype(BF16)


def spread_kernel(parts_ref, out_ref, pos_ref):
    def put(index, tile):
        out_ref[:, index, :, :] = jnp.broadcast_to(tile[None], (TGT, ROWS, LANES))

    mixed = [parts_ref[source, 3, :, :].astype(F32) for source in range(SLICES)]
    pos = group_lanes(mixed, POS_LANE)
    pos_ref[...] = pos
    for source in range(SLICES):
        for index in range(3):
            put(3 * source + index, parts_ref[source, index, :, :])
    lane = lax.broadcasted_iota(jnp.int32, (ROWS, LANES), 1)
    for pair in range(SLICES // 2):
        left = pltpu.roll(mixed[2 * pair], LANES - MIX_LANE, 1)
        right = pltpu.roll(mixed[2 * pair + 1], HALF_ROW - MIX_LANE, 1)
        put(CHARGE_TILE + pair, jnp.where(lane < HALF_ROW, left, right).astype(BF16))
    put(LAST_TILE, group_lanes(mixed, 0))
    put(POS_TILE, pos)


def main_kernel(
    count_hbm,
    feats_ref,
    group_ref,
    out_ref,
    src_ref,
    tgt_ref,
    coef_ref,
    xt_ref,
    rows_ref,
    yt_ref,
    acc_ref,
    list_ref,
    count_ref,
    sem,
):
    zone = lax.axis_index("zh")
    target_group = lax.axis_index("tgt")
    count_copy = pltpu.make_async_copy(count_hbm, count_ref, sem)
    count_copy.start()

    spare = pl.ds(ROWS * SLICES, ROWS)
    src_ref[spare, :] = jnp.zeros((ROWS, LANES), F32)
    tgt_ref[spare, :] = jnp.full((ROWS, LANES), SRC * ROWS, F32)
    for index in range(17):
        coef_ref[index, spare, :] = jnp.zeros((ROWS, LANES), F32)
    for tile in range(SLICES):
        rows = pl.ds(ROWS * tile, ROWS)
        src_ref[rows, :] = group_ref[tile, 4, :, :].astype(F32)
        tgt_ref[rows, :] = group_ref[tile, 5, :, :].astype(F32)
        angle = group_ref[tile, 6, :, :].astype(F32) + group_ref[tile, 7, :, :].astype(F32)
        scale = group_ref[tile, 8, :, :].astype(F32) * math.sqrt(0.5)
        c1, s1 = sincos_turns(angle * (0.5 / math.pi))
        c, s = c1, s1
        coef_ref[16, rows, :] = scale
        for order in range(4):
            if order:
                c, s = c * c1 - s * s1, s * c1 + c * s1
            coef_ref[4 * order, rows, :] = c
            coef_ref[4 * order + 1, rows, :] = s
            coef_ref[4 * order + 2, rows, :] = scale * c
            coef_ref[4 * order + 3, rows, :] = scale * s
    last = feats_ref[:, LAST_TILE, :, :].reshape(TGT * ROWS, LANES).T
    for tile in range(SLICES):
        for index in range(3):
            block = feats_ref[:, 3 * tile + index, :, :].reshape(TGT * ROWS, LANES)
            xt_ref[tile, index * LANES : (index + 1) * LANES, :] = block.T
        xt_ref[tile, 3 * LANES :, :] = last[tile * CH : (tile + 1) * CH]

    count_copy.wait()
    per_step = STEP // LANES

    def list_tile(tile, at):
        source = (tile // R) * (ZH * R) + zone * R + tile % R
        steps = (count_ref[target_group, source] + STEP - 1) // STEP

        def put(step, place):
            list_ref[place] = tile * ROWS + step * per_step
            return place + 1

        return lax.fori_loop(0, steps, put, at)

    for place in range(2):
        list_ref[place] = ROWS * SLICES
    end = lax.fori_loop(0, SLICES, list_tile, 2)
    for extra in range(3):
        list_ref[end + extra] = ROWS * SLICES
    pairs = (end - 1) // 2

    acc_ref[...] = jnp.zeros_like(acc_ref)
    yt_ref[...] = jnp.zeros_like(yt_ref)
    src_ids = lax.broadcasted_iota(jnp.int32, (TGT * ROWS, STEP), 0).astype(F32)
    tgt_ids = lax.broadcasted_iota(jnp.int32, (SRC * ROWS, 2 * STEP), 0).astype(F32).astype(BF16)

    def lanes_of(rows, ref, *lead):
        return jnp.concatenate(
            [ref[(*lead, pl.ds(row + part, 1), slice(None))] for row in rows for part in range(per_step)], axis=1
        )

    def gather(rows, part):
        kept = slice(part * HALF, (part + 1) * HALF if part == 0 else COLS)
        for half, row in enumerate(rows):
            tile = jnp.minimum(row // ROWS, SLICES - 1)
            one_src = (src_ids == lanes_of([row], src_ref)).astype(F32).astype(BF16)
            rows_ref[kept, half * STEP : (half + 1) * STEP] = jnp.dot(
                xt_ref[tile, kept, :], one_src, preferred_element_type=F32
            )

    def convert(rows, order):
        offset, blocks = SPANS[order]
        if order == 0:
            scale = lanes_of(rows, coef_ref, 16)
            for low in range(0, blocks * CH, CH):
                gathered = rows_ref[low : low + CH, :]
                yt_ref[low : low + CH, :] = ((gathered + gathered * lax.erf(gathered)) * scale).astype(BF16)
            return
        cos_in, sin_in, cos_out, sin_out = (lanes_of(rows, coef_ref, 4 * (order - 1) + part) for part in range(4))
        for block in range(blocks):
            low = (offset + block) * CH
            high = low + blocks * CH
            lead, trail = rows_ref[low : low + CH, :], rows_ref[high : high + CH, :]
            lead, trail = cos_in * lead + sin_in * trail, cos_in * trail - sin_in * lead
            lead, trail = lead + lead * lax.erf(lead), trail + trail * lax.erf(trail)
            yt_ref[low : low + CH, :] = (cos_out * lead - sin_out * trail).astype(BF16)
            yt_ref[high : high + CH, :] = (cos_out * trail + sin_out * lead).astype(BF16)

    def scatter(rows, part):
        columns = slice(part * CUT, min((part + 1) * CUT, COLS))
        one_tgt = jnp.where(tgt_ids == lanes_of(rows, tgt_ref).astype(BF16), jnp.ones((), BF16), jnp.zeros((), BF16))
        acc_ref[:, columns] += lax.dot_general(
            one_tgt, yt_ref[columns, :], (((1,), (1,)), ((), ())), preferred_element_type=F32
        )

    def two_rows(pair):
        return [list_ref[2 * pair], list_ref[2 * pair + 1]]

    def one_pair(pair, carry):
        before, now, then = (two_rows(pair + part) for part in range(3))
        scatter(before, 0)
        for order in (4, 3, 2):
            convert(now, order)
        gather(then, 1)
        scatter(now, 1)
        for order in (0, 1):
            convert(now, order)
        gather(then, 0)
        return carry

    for part in range(2):
        gather(two_rows(1), part)
    lax.fori_loop(0, pairs, one_pair, 0)
    scatter(two_rows(pairs), 0)
    for index in range(4):
        out_ref[:, index, :, :] = (
            acc_ref[:, index * LANES : (index + 1) * LANES].reshape(SRC, ROWS, LANES).astype(BF16)
        )


EVEN_ODD = (*range(0, SLICES, 2), *range(1, SLICES, 2))


def spread_positions(packed, sources):
    packed = packed.astype(F32)
    tiles = [pltpu.roll(packed, LANES - CH * index, 1) if index else packed for index in sources]
    return jnp.concatenate(tiles, axis=0).astype(BF16)


def message_kernel(feats_ref, pos_ref0, pos_ref1, pos_ref2, pos_ref3, kidx_ref, kfilter_ref, parts_ref, out_ref):
    zone = lax.axis_index("zh")
    kslice = kfilter_ref.shape[0] // K_SLICES
    k_start = pl.multiple_of(k_slice_index() * kslice, kslice)
    row_ids = lax.broadcasted_iota(jnp.int32, (LANES, kslice), 0)
    k_rows = kidx_ref[:, pl.ds(k_start, kslice)].astype(F32)
    k_table = jnp.zeros((LANES, kslice), F32)
    for axis in range(3):
        k_table = jnp.where((row_ids >= 3 * axis) & (row_ids < 3 * axis + 3), k_rows[axis : axis + 1, :], k_table)
    charges = jnp.concatenate(
        [feats_ref[:, CHARGE_TILE + pair, :, :].reshape(TGT * ROWS, LANES) for pair in range(SLICES // 2)], axis=0
    )
    atoms = charges.shape[0]
    turns = lax.dot_general(
        k_table.T.astype(BF16),
        spread_positions(feats_ref[:, POS_TILE, :, :].reshape(TGT * ROWS, LANES), EVEN_ODD),
        (((1,), (1,)), ((), ())),
        preferred_element_type=F32,
    )
    own_pos = jnp.concatenate(
        [spread_positions(ref[...], range(SLICES)) for ref in (pos_ref0, pos_ref1, pos_ref2, pos_ref3)], axis=0
    )
    own_turns = jnp.dot(own_pos, k_table.astype(BF16), preferred_element_type=F32)
    filters = kfilter_ref[pl.ds(k_start, kslice), :]
    filters = jnp.where(lax.axis_index("r") % 2 == 1, pltpu.roll(filters, HALF_ROW, 1), filters)
    total = jnp.zeros((SRC * ROWS, LANES), F32)
    for table, own_table in zip(sincos_turns(turns), sincos_turns(own_turns)):
        table = table.astype(BF16)
        even = jnp.dot(table[:, :atoms], charges, preferred_element_type=F32)
        odd = jnp.dot(table[:, atoms:], charges, preferred_element_type=F32)
        own_table = own_table.astype(BF16)
        for part in split2(filters * (even + pltpu.roll(odd, HALF_ROW, 1))):
            total = total + jnp.dot(own_table, part, preferred_element_type=F32)
    total = in_mix(pltpu.roll(total, MIX_LANE, 1))
    for shift in range(ZH):
        from_zone = (zone + ZH - shift) % ZH
        for y in range(Y):
            low = (shift * SLICES + y * R) * ROWS
            place = pl.ds(y * ZH * R + from_zone * R, R)
            out_ref[place, :3, :, :] = parts_ref[place, :3, :, :]
            out_ref[place, 3, :, :] = (
                parts_ref[place, 3, :, :].astype(F32) + total[low : low + R * ROWS].reshape(R, ROWS, LANES)
            ).astype(BF16)


def last_conv_kernel(norm, parts_ref, w0, w1, w2, w3, w4, update_ref, long_ref, conv_ref):
    halves = []
    for half in range(2):
        total = jnp.zeros((ROWS, LANES), F32)
        for source in range(half, SRC, 2):
            total = total + parts_ref[source, 3, :, :].astype(F32)
        halves.append(pltpu.roll(total, (HALF_ROW * half - MIX_LANE) % LANES, 1))
    lane = lax.broadcasted_iota(jnp.int32, (ROWS, LANES), 1)
    long_ref[...] = jnp.where(lane < HALF_ROW, *halves) * norm
    place = lax.broadcasted_iota(jnp.int32, (ROWS, LANES), 1) // CH
    for index in range(4):
        sums = []
        for piece in range(SLICES):
            total = jnp.zeros((ROWS, LANES), F32)
            for zone in range(ZH):
                source = (piece // R) * (ZH * R) + zone * R + piece % R
                total = total + parts_ref[source, index, :, :].astype(F32)
            sums.append(total)
        for within in range(min(8, BLOCKS - 8 * index)):
            block = 8 * index + within
            tile = jnp.zeros((ROWS, LANES), F32)
            for piece in range(SLICES):
                moved = sums[piece]
                if within != piece:
                    moved = pltpu.roll(moved, (CH * (piece - within)) % LANES, 1)
                tile = jnp.where(place == piece, moved, tile)
            conv_ref[:, block * LANES : (block + 1) * LANES] = tile
    width = SPANS[0][1] * LANES
    value = conv_ref[:, :width]
    rounded = value.astype(BF16).astype(F32)
    stacked = jnp.concatenate([rounded, value - rounded], axis=0).astype(BF16)
    product = jnp.dot(stacked, w0[1], preferred_element_type=F32)
    update_ref[:, :width] = (product[:ROWS] + product[ROWS:]).astype(BF16)
    for order, weight in zip(range(1, 5), (w1, w2, w3, w4)):
        offset, blocks = SPANS[order]
        start, width = offset * LANES, blocks * LANES
        lead, trail = conv_ref[:, start : start + width], conv_ref[:, start + width : start + 2 * width]
        lead_high, trail_high = lead.astype(BF16).astype(F32), trail.astype(BF16).astype(F32)
        stacked = jnp.concatenate([lead_high, trail_high, lead - lead_high, trail - trail_high], axis=0)
        lead, trail = pair_product(stacked.astype(BF16), weight.at[1])
        update_ref[:, start : start + width] = lead.astype(BF16)
        update_ref[:, start + width : start + 2 * width] = trail.astype(BF16)


def params(mib):
    return pltpu.CompilerParams(vmem_limit_bytes=mib << 20)


def body(
    atom_feats,
    positions,
    edge_src,
    edge_tgt,
    edge_angle,
    edge_scale,
    edge_count,
    k_index,
    k_filter,
    *weights,
):
    slots = edge_src.shape[0]
    columns = atom_feats.shape[1]
    tile_shape = (ROWS, slots // ROWS)
    vmem = pl.BlockSpec(memory_space=pltpu.VMEM)
    hbm = pl.BlockSpec(memory_space=pltpu.HBM)
    counts = edge_count.T
    group_out = (SLICES, 9, ROWS, LANES)
    sources = (atom_feats, positions) + tuple(
        value.reshape(tile_shape) for value in (edge_src, edge_tgt, edge_angle, edge_scale)
    )
    group = pl.pallas_call(
        first_kernel,
        out_shape=jax.ShapeDtypeStruct(group_out, BF16),
        in_specs=[hbm] * 12,
        out_specs=vmem,
        scratch_shapes=[pltpu.VMEM(value.shape, value.dtype) for value in sources]
        + [pltpu.VMEM(weight.shape[1:], weight.dtype) for weight in weights]
        + [pltpu.VMEM((ROWS, columns), F32), pltpu.SMEM(counts.shape, jnp.int32), pltpu.SemaphoreType.DMA((12,))],
        compiler_params=params(56),
        cost_estimate=COST["first"],
        name="first",
    )(counts, *sources, *weights)
    group = lax.all_to_all(group, ("y", "r"), 0, 0)
    feats_out = (TGT, TILES, ROWS, LANES)
    pos_out = (ROWS, LANES)
    feats, pos = pl.pallas_call(
        spread_kernel,
        out_shape=(jax.ShapeDtypeStruct(feats_out, BF16), jax.ShapeDtypeStruct(pos_out, BF16)),
        in_specs=[vmem],
        out_specs=(vmem, vmem),
        compiler_params=params(32),
        cost_estimate=COST["spread"],
        name="spread",
    )(group)
    feats = lax.all_to_all(feats, "tgt", 0, 0)
    zones = [pos]
    for shift in range(1, ZH):
        zones.append(lax.ppermute(pos, "zh", [(i, (i + shift) % ZH) for i in range(ZH)]))

    parts_out = (SRC, 4, ROWS, LANES)
    parts = pl.pallas_call(
        main_kernel,
        out_shape=jax.ShapeDtypeStruct(parts_out, BF16),
        in_specs=[hbm, vmem, vmem],
        out_specs=vmem,
        scratch_shapes=[
            pltpu.VMEM(((SLICES + 1) * ROWS, LANES), F32),
            pltpu.VMEM(((SLICES + 1) * ROWS, LANES), F32),
            pltpu.VMEM((17, (SLICES + 1) * ROWS, LANES), F32),
            pltpu.VMEM((SLICES, COLS, TGT * ROWS), BF16),
            pltpu.VMEM((COLS, 2 * STEP), F32),
            pltpu.VMEM((COLS, 2 * STEP), BF16),
            pltpu.VMEM((SRC * ROWS, 4 * LANES), F32),
            pltpu.SMEM((SLICES * (slots // STEP) + 5,), jnp.int32),
            pltpu.SMEM(counts.shape, jnp.int32),
            pltpu.SemaphoreType.DMA,
        ],
        compiler_params=params(32),
        cost_estimate=COST["edge_sums"],
        name="edge_sums",
    )(counts, feats, group)
    parts = pl.pallas_call(
        message_kernel,
        out_shape=jax.ShapeDtypeStruct(parts_out, BF16),
        in_specs=[vmem] * 8,
        out_specs=vmem,
        compiler_params=params(32),
        cost_estimate=COST["message"],
        name="message",
    )(feats, *zones, k_index, k_filter, parts)
    parts = lax.all_to_all(parts, SRC_AXES, 0, 0)

    norm = 1.0 / math.sqrt(SRC * TGT * ROWS * k_index.shape[1])
    return pl.pallas_call(
        lambda *refs: last_conv_kernel(norm, *refs),
        out_shape=(
            jax.ShapeDtypeStruct((ROWS, columns), BF16),
            jax.ShapeDtypeStruct((ROWS, LANES), F32),
        ),
        in_specs=[vmem] * 6,
        out_specs=(vmem, vmem),
        scratch_shapes=[pltpu.VMEM((ROWS, columns), F32)],
        compiler_params=params(16),
        cost_estimate=COST["last_conv"],
        name="last_conv",
    )(parts, *weights)


def solution(mesh):
    fine = Mesh(mesh.devices.reshape(Y, ZH, R, TGT), ALL_AXES)
    return jax.shard_map(
        body,
        mesh=fine,
        in_specs=(P(ALL_AXES, None), P(None, ALL_AXES)) + (P(ALL_AXES),) * 4 + (P(),) * 8,
        out_specs=(P(("tgt",) + SRC_AXES, None), P(ALL_AXES, None)),
        check_vma=False,
    )
```

```python
import math

import jax
import jax.numpy as jnp
from jax import lax
from jax.experimental import pallas as pl
from jax.experimental.pallas import tpu as pltpu
from jax.sharding import Mesh
from jax.sharding import PartitionSpec as P

Y, ZH, R, TGT = 2, 4, 4, 8
SRC_AXES = ("y", "zh", "r")
ALL_AXES = ("y", "zh", "r", "tgt")
SRC = Y * ZH * R
SLICES = Y * R
LANES = 128
ROWS = 8
BLOCKS = 25
CH = LANES // SLICES
COLS = BLOCKS * CH
HALF = 208
CUT = 256
STEP = 256
POS_LANE = 16
MIX_LANE = 32
HALF_ROW = LANES // 2
K_SLICES = SLICES // 2
LAST_TILE, POS_TILE, CHARGE_TILE, TILES = 24, 25, 26, 30
COST = {
    "first": pl.CostEstimate(flops=50_000_000, transcendentals=0, bytes_accessed=3_000_000),
    "spread": pl.CostEstimate(flops=0, transcendentals=0, bytes_accessed=800_000),
    "edge_sums": pl.CostEstimate(flops=8_000_000_000, transcendentals=1_500_000, bytes_accessed=2_000_000),
    "message": pl.CostEstimate(flops=3_000_000_000, transcendentals=400_000, bytes_accessed=1_000_000),
    "last_conv": pl.CostEstimate(flops=100_000_000, transcendentals=0, bytes_accessed=3_200_000),
}
F32 = jnp.float32
BF16 = jnp.bfloat16


def order_spans():
    spans = [(0, 5)]
    offset = 5
    for order in range(1, 5):
        spans.append((offset, 5 - order))
        offset += 2 * (5 - order)
    return spans


SPANS = order_spans()


SIN_TERMS = (4.442867903, -7.307443419, 3.59478806, -0.7843739803)
COS_TERMS = (1.414213497, -6.978850988, 5.739461171, -1.88356299, 0.3106981923)


def series(terms, x2):
    value = terms[-1]
    for term in terms[-2::-1]:
        value = value * x2 + term
    return value


def sincos_turns(turns):
    part = turns - jnp.round(turns)
    x2 = part * part
    s = part * series(SIN_TERMS, x2)
    return 1.0 - s * s, s * series(COS_TERMS, x2)


def position_tile(pos_ref):
    row_ids = lax.broadcasted_iota(jnp.int32, (ROWS, ROWS), 0)
    col_ids = lax.broadcasted_iota(jnp.int32, (ROWS, ROWS), 1)
    lane = lax.broadcasted_iota(jnp.int32, (ROWS, LANES), 1)
    tile = jnp.zeros((ROWS, LANES), F32)
    for axis in range(3):
        spread = jnp.broadcast_to(pos_ref[axis : axis + 1, :], (ROWS, ROWS))
        rest = jnp.sum(jnp.where(row_ids == col_ids, spread, 0.0), axis=1, keepdims=True)
        for part in range(3):
            piece = rest.astype(BF16).astype(F32)
            rest = rest - piece
            tile = jnp.where(lane == POS_LANE + 3 * axis + part, piece, tile)
    return tile


def edge_tiles(count_ref, src_ref, tgt_ref, angle_ref, scale_ref):
    group = (lax.axis_index("y") * ZH + lax.axis_index("zh")) * R + lax.axis_index("r")
    count = count_ref[lax.axis_index("tgt"), group]
    slot = lax.broadcasted_iota(jnp.int32, (ROWS, LANES), 0) * LANES + lax.broadcasted_iota(
        jnp.int32, (ROWS, LANES), 1
    )
    angle = angle_ref[...]
    angle_high = angle.astype(BF16).astype(F32)
    return (
        src_ref[...].astype(F32),
        jnp.where(slot < count, tgt_ref[...], SRC * ROWS).astype(F32),
        angle_high,
        angle - angle_high,
        scale_ref[...],
    )


def pair_product(stacked, weight_ref):
    first = jnp.dot(stacked, weight_ref[0], preferred_element_type=F32)
    second = jnp.dot(stacked, weight_ref[1], preferred_element_type=F32)
    lead = jnp.zeros((ROWS, first.shape[1]), F32)
    trail = lead
    for base in range(0, stacked.shape[0], 2 * ROWS):
        lead = lead + (first[base : base + ROWS] - second[base + ROWS : base + 2 * ROWS])
        trail = trail + (second[base : base + ROWS] + first[base + ROWS : base + 2 * ROWS])
    return lead, trail


def k_slice_index():
    return lax.axis_index("y") * (R // 2) + lax.axis_index("r") // 2


def in_mix(value):
    lane = lax.broadcasted_iota(jnp.int32, value.shape, value.ndim - 1)
    return jnp.where((lane >= MIX_LANE) & (lane < MIX_LANE + HALF_ROW), value, 0.0)


def first_kernel(count_hbm, *refs):
    sources, out_ref, held, (conv_ref, count_ref, sems) = refs[:11], refs[11], refs[12:23], refs[23:]
    copies = [
        pltpu.make_async_copy(source if index < 6 else source.at[0], to, sems.at[index])
        for index, (source, to) in enumerate(zip(sources, held))
    ]
    count_copy = pltpu.make_async_copy(count_hbm, count_ref, sems.at[11])
    count_copy.start()
    for copy in copies:
        copy.start()
    feats_ref, pos_ref = held[0], held[1]
    for copy in copies[:6]:
        copy.wait()
    pos = position_tile(pos_ref)
    count_copy.wait()
    for index, tile in enumerate(edge_tiles(count_ref, *held[2:6])):
        out_ref[:, 4 + index, :, :] = jnp.broadcast_to(tile.astype(BF16)[None], (SLICES, ROWS, LANES))
    x = feats_ref[...].astype(F32)
    mixed = [pos + in_mix(pltpu.roll(x[:, :LANES], (MIX_LANE - HALF_ROW * half) % LANES, 1)) for half in range(2)]
    place = lax.broadcasted_iota(jnp.int32, (ROWS, LANES), 1) // CH

    def emit(tile_index):
        for piece in range(SLICES):
            tile = mixed[piece % 2] if tile_index == 3 else jnp.zeros((ROWS, LANES), F32)
            for within in range(min(8, BLOCKS - 8 * tile_index)):
                block = 8 * tile_index + within
                moved = conv_ref[:, block * LANES : (block + 1) * LANES]
                if within != piece:
                    moved = pltpu.roll(moved, (CH * (within - piece)) % LANES, 1)
                tile = jnp.where(place == within, moved, tile)
            out_ref[piece, tile_index, :, :] = tile.astype(BF16)

    root = math.sqrt(0.5)
    for order in range(5):
        copies[6 + order].wait()
        weight = held[6 + order]
        offset, blocks = SPANS[order]
        start, width = offset * LANES, blocks * LANES
        if order == 0:
            conv_ref[:, :width] = root * jnp.dot(x[:, :width].astype(BF16), weight[...], preferred_element_type=F32)
            continue
        stacked = jnp.concatenate([x[:, start : start + width], x[:, start + width : start + 2 * width]], axis=0)
        lead, trail = pair_product(stacked.astype(BF16), weight)
        conv_ref[:, start : start + width] = root * lead
        conv_ref[:, start + width : start + 2 * width] = root * trail
    for tile_index in range(4):
        emit(tile_index)


def group_lanes(tiles, first_lane):
    place = lax.broadcasted_iota(jnp.int32, (ROWS, LANES), 1) // CH
    packed = jnp.zeros((ROWS, LANES), F32)
    for index, tile in enumerate(tiles):
        shift = (CH * index - first_lane) % LANES
        packed = jnp.where(place == index, pltpu.roll(tile, shift, 1) if shift else tile, packed)
    return packed.astype(BF16)


def spread_kernel(parts_ref, out_ref, pos_ref):
    def put(index, tile):
        out_ref[:, index, :, :] = jnp.broadcast_to(tile[None], (TGT, ROWS, LANES))

    mixed = [parts_ref[source, 3, :, :].astype(F32) for source in range(SLICES)]
    pos = group_lanes(mixed, POS_LANE)
    pos_ref[...] = pos
    for source in range(SLICES):
        for index in range(3):
            put(3 * source + index, parts_ref[source, index, :, :])
    lane = lax.broadcasted_iota(jnp.int32, (ROWS, LANES), 1)
    for pair in range(SLICES // 2):
        left = pltpu.roll(mixed[2 * pair], LANES - MIX_LANE, 1)
        right = pltpu.roll(mixed[2 * pair + 1], HALF_ROW - MIX_LANE, 1)
        put(CHARGE_TILE + pair, jnp.where(lane < HALF_ROW, left, right).astype(BF16))
    put(LAST_TILE, group_lanes(mixed, 0))
    put(POS_TILE, pos)


def main_kernel(
    count_hbm,
    feats_ref,
    group_ref,
    out_ref,
    src_ref,
    tgt_ref,
    coef_ref,
    xt_ref,
    rows_ref,
    yt_ref,
    acc_ref,
    list_ref,
    count_ref,
    sem,
):
    zone = lax.axis_index("zh")
    target_group = lax.axis_index("tgt")
    count_copy = pltpu.make_async_copy(count_hbm, count_ref, sem)
    count_copy.start()

    spare = pl.ds(ROWS * SLICES, ROWS)
    src_ref[spare, :] = jnp.zeros((ROWS, LANES), F32)
    tgt_ref[spare, :] = jnp.full((ROWS, LANES), SRC * ROWS, F32)
    for index in range(17):
        coef_ref[index, spare, :] = jnp.zeros((ROWS, LANES), F32)
    for tile in range(SLICES):
        rows = pl.ds(ROWS * tile, ROWS)
        src_ref[rows, :] = group_ref[tile, 4, :, :].astype(F32)
        tgt_ref[rows, :] = group_ref[tile, 5, :, :].astype(F32)
        angle = group_ref[tile, 6, :, :].astype(F32) + group_ref[tile, 7, :, :].astype(F32)
        scale = group_ref[tile, 8, :, :].astype(F32) * math.sqrt(0.5)
        c1, s1 = sincos_turns(angle * (0.5 / math.pi))
        c, s = c1, s1
        coef_ref[16, rows, :] = scale
        for order in range(4):
            if order:
                c, s = c * c1 - s * s1, s * c1 + c * s1
            coef_ref[4 * order, rows, :] = c
            coef_ref[4 * order + 1, rows, :] = s
            coef_ref[4 * order + 2, rows, :] = scale * c
            coef_ref[4 * order + 3, rows, :] = scale * s
    last = feats_ref[:, LAST_TILE, :, :].reshape(TGT * ROWS, LANES).T
    for tile in range(SLICES):
        for index in range(3):
            block = feats_ref[:, 3 * tile + index, :, :].reshape(TGT * ROWS, LANES)
            xt_ref[tile, index * LANES : (index + 1) * LANES, :] = block.T
        xt_ref[tile, 3 * LANES :, :] = last[tile * CH : (tile + 1) * CH]

    count_copy.wait()
    per_step = STEP // LANES

    def list_tile(tile, at):
        source = (tile // R) * (ZH * R) + zone * R + tile % R
        steps = (count_ref[target_group, source] + STEP - 1) // STEP

        def put(step, place):
            list_ref[place] = tile * ROWS + step * per_step
            return place + 1

        return lax.fori_loop(0, steps, put, at)

    for place in range(2):
        list_ref[place] = ROWS * SLICES
    end = lax.fori_loop(0, SLICES, list_tile, 2)
    for extra in range(3):
        list_ref[end + extra] = ROWS * SLICES
    pairs = (end - 1) // 2

    acc_ref[...] = jnp.zeros_like(acc_ref)
    yt_ref[...] = jnp.zeros_like(yt_ref)
    src_ids = lax.broadcasted_iota(jnp.int32, (TGT * ROWS, STEP), 0).astype(F32)
    tgt_ids = lax.broadcasted_iota(jnp.int32, (SRC * ROWS, 2 * STEP), 0).astype(F32).astype(BF16)

    def lanes_of(rows, ref, *lead):
        return jnp.concatenate(
            [ref[(*lead, pl.ds(row + part, 1), slice(None))] for row in rows for part in range(per_step)], axis=1
        )

    def gather(rows, part):
        kept = slice(part * HALF, (part + 1) * HALF if part == 0 else COLS)
        for half, row in enumerate(rows):
            tile = jnp.minimum(row // ROWS, SLICES - 1)
            one_src = (src_ids == lanes_of([row], src_ref)).astype(F32).astype(BF16)
            rows_ref[kept, half * STEP : (half + 1) * STEP] = jnp.dot(
                xt_ref[tile, kept, :], one_src, preferred_element_type=F32
            )

    def convert(rows, order):
        offset, blocks = SPANS[order]
        if order == 0:
            scale = lanes_of(rows, coef_ref, 16)
            for low in range(0, blocks * CH, CH):
                gathered = rows_ref[low : low + CH, :]
                yt_ref[low : low + CH, :] = ((gathered + gathered * lax.erf(gathered)) * scale).astype(BF16)
            return
        cos_in, sin_in, cos_out, sin_out = (lanes_of(rows, coef_ref, 4 * (order - 1) + part) for part in range(4))
        for block in range(blocks):
            low = (offset + block) * CH
            high = low + blocks * CH
            lead, trail = rows_ref[low : low + CH, :], rows_ref[high : high + CH, :]
            lead, trail = cos_in * lead + sin_in * trail, cos_in * trail - sin_in * lead
            lead, trail = lead + lead * lax.erf(lead), trail + trail * lax.erf(trail)
            yt_ref[low : low + CH, :] = (cos_out * lead - sin_out * trail).astype(BF16)
            yt_ref[high : high + CH, :] = (cos_out * trail + sin_out * lead).astype(BF16)

    def scatter(rows, part):
        columns = slice(part * CUT, min((part + 1) * CUT, COLS))
        one_tgt = jnp.where(tgt_ids == lanes_of(rows, tgt_ref).astype(BF16), jnp.ones((), BF16), jnp.zeros((), BF16))
        acc_ref[:, columns] += lax.dot_general(
            one_tgt, yt_ref[columns, :], (((1,), (1,)), ((), ())), preferred_element_type=F32
        )

    def two_rows(pair):
        return [list_ref[2 * pair], list_ref[2 * pair + 1]]

    def one_pair(pair, carry):
        before, now, then = (two_rows(pair + part) for part in range(3))
        scatter(before, 0)
        for order in (4, 3, 2):
            convert(now, order)
        gather(then, 1)
        scatter(now, 1)
        for order in (0, 1):
            convert(now, order)
        gather(then, 0)
        return carry

    for part in range(2):
        gather(two_rows(1), part)
    lax.fori_loop(0, pairs, one_pair, 0)
    scatter(two_rows(pairs), 0)
    for index in range(4):
        out_ref[:, index, :, :] = (
            acc_ref[:, index * LANES : (index + 1) * LANES].reshape(SRC, ROWS, LANES).astype(BF16)
        )


EVEN_ODD = (*range(0, SLICES, 2), *range(1, SLICES, 2))


def spread_positions(packed, sources):
    packed = packed.astype(F32)
    tiles = [pltpu.roll(packed, LANES - CH * index, 1) if index else packed for index in sources]
    return jnp.concatenate(tiles, axis=0).astype(BF16)


def message_kernel(feats_ref, pos_ref0, pos_ref1, pos_ref2, pos_ref3, kidx_ref, kfilter_ref, parts_ref, out_ref):
    zone = lax.axis_index("zh")
    kslice = kfilter_ref.shape[0] // K_SLICES
    k_start = pl.multiple_of(k_slice_index() * kslice, kslice)
    row_ids = lax.broadcasted_iota(jnp.int32, (LANES, kslice), 0)
    k_rows = kidx_ref[:, pl.ds(k_start, kslice)].astype(F32)
    k_table = jnp.zeros((LANES, kslice), F32)
    for axis in range(3):
        k_table = jnp.where((row_ids >= 3 * axis) & (row_ids < 3 * axis + 3), k_rows[axis : axis + 1, :], k_table)
    charges = jnp.concatenate(
        [feats_ref[:, CHARGE_TILE + pair, :, :].reshape(TGT * ROWS, LANES) for pair in range(SLICES // 2)], axis=0
    )
    atoms = charges.shape[0]
    turns = lax.dot_general(
        k_table.T.astype(BF16),
        spread_positions(feats_ref[:, POS_TILE, :, :].reshape(TGT * ROWS, LANES), EVEN_ODD),
        (((1,), (1,)), ((), ())),
        preferred_element_type=F32,
    )
    own_pos = jnp.concatenate(
        [spread_positions(ref[...], range(SLICES)) for ref in (pos_ref0, pos_ref1, pos_ref2, pos_ref3)], axis=0
    )
    own_turns = jnp.dot(own_pos, k_table.astype(BF16), preferred_element_type=F32)
    filters = kfilter_ref[pl.ds(k_start, kslice), :]
    filters = jnp.where(lax.axis_index("r") % 2 == 1, pltpu.roll(filters, HALF_ROW, 1), filters)
    total = jnp.zeros((SRC * ROWS, LANES), F32)
    for table, own_table in zip(sincos_turns(turns), sincos_turns(own_turns)):
        table = table.astype(BF16)
        even = jnp.dot(table[:, :atoms], charges, preferred_element_type=F32)
        odd = jnp.dot(table[:, atoms:], charges, preferred_element_type=F32)
        own_table = own_table.astype(BF16)
        factors = (filters * (even + pltpu.roll(odd, HALF_ROW, 1))).astype(BF16)
        total = total + jnp.dot(own_table, factors, preferred_element_type=F32)
    total = in_mix(pltpu.roll(total, MIX_LANE, 1))
    for shift in range(ZH):
        from_zone = (zone + ZH - shift) % ZH
        for y in range(Y):
            low = (shift * SLICES + y * R) * ROWS
            place = pl.ds(y * ZH * R + from_zone * R, R)
            out_ref[place, 3, :, :] = (
                parts_ref[place, 3, :, :].astype(F32) + total[low : low + R * ROWS].reshape(R, ROWS, LANES)
            ).astype(BF16)


def last_conv_kernel(norm, parts_ref, w0, w1, w2, w3, w4, update_ref, long_ref, conv_ref):
    halves = []
    for half in range(2):
        total = jnp.zeros((ROWS, LANES), F32)
        for source in range(half, SRC, 2):
            total = total + parts_ref[source, 3, :, :].astype(F32)
        halves.append(pltpu.roll(total, (HALF_ROW * half - MIX_LANE) % LANES, 1))
    lane = lax.broadcasted_iota(jnp.int32, (ROWS, LANES), 1)
    long_ref[...] = jnp.where(lane < HALF_ROW, *halves) * norm
    place = lax.broadcasted_iota(jnp.int32, (ROWS, LANES), 1) // CH
    for index in range(4):
        sums = []
        for piece in range(SLICES):
            total = jnp.zeros((ROWS, LANES), F32)
            for zone in range(ZH):
                source = (piece // R) * (ZH * R) + zone * R + piece % R
                total = total + parts_ref[source, index, :, :].astype(F32)
            sums.append(total)
        for within in range(min(8, BLOCKS - 8 * index)):
            block = 8 * index + within
            tile = jnp.zeros((ROWS, LANES), F32)
            for piece in range(SLICES):
                moved = sums[piece]
                if within != piece:
                    moved = pltpu.roll(moved, (CH * (piece - within)) % LANES, 1)
                tile = jnp.where(place == piece, moved, tile)
            conv_ref[:, block * LANES : (block + 1) * LANES] = tile
    width = SPANS[0][1] * LANES
    value = conv_ref[:, :width]
    rounded = value.astype(BF16).astype(F32)
    stacked = jnp.concatenate([rounded, value - rounded], axis=0).astype(BF16)
    product = jnp.dot(stacked, w0[1], preferred_element_type=F32)
    update_ref[:, :width] = (product[:ROWS] + product[ROWS:]).astype(BF16)
    for order, weight in zip(range(1, 5), (w1, w2, w3, w4)):
        offset, blocks = SPANS[order]
        start, width = offset * LANES, blocks * LANES
        lead, trail = conv_ref[:, start : start + width], conv_ref[:, start + width : start + 2 * width]
        lead_high, trail_high = lead.astype(BF16).astype(F32), trail.astype(BF16).astype(F32)
        stacked = jnp.concatenate([lead_high, trail_high, lead - lead_high, trail - trail_high], axis=0)
        lead, trail = pair_product(stacked.astype(BF16), weight.at[1])
        update_ref[:, start : start + width] = lead.astype(BF16)
        update_ref[:, start + width : start + 2 * width] = trail.astype(BF16)


def params(mib):
    return pltpu.CompilerParams(vmem_limit_bytes=mib << 20)


def body(
    atom_feats,
    positions,
    edge_src,
    edge_tgt,
    edge_angle,
    edge_scale,
    edge_count,
    k_index,
    k_filter,
    *weights,
):
    slots = edge_src.shape[0]
    columns = atom_feats.shape[1]
    tile_shape = (ROWS, slots // ROWS)
    vmem = pl.BlockSpec(memory_space=pltpu.VMEM)
    hbm = pl.BlockSpec(memory_space=pltpu.HBM)
    counts = edge_count.T
    group_out = (SLICES, 9, ROWS, LANES)
    sources = (atom_feats, positions) + tuple(
        value.reshape(tile_shape) for value in (edge_src, edge_tgt, edge_angle, edge_scale)
    )
    group = pl.pallas_call(
        first_kernel,
        out_shape=jax.ShapeDtypeStruct(group_out, BF16),
        in_specs=[hbm] * 12,
        out_specs=vmem,
        scratch_shapes=[pltpu.VMEM(value.shape, value.dtype) for value in sources]
        + [pltpu.VMEM(weight.shape[1:], weight.dtype) for weight in weights]
        + [pltpu.VMEM((ROWS, columns), F32), pltpu.SMEM(counts.shape, jnp.int32), pltpu.SemaphoreType.DMA((12,))],
        compiler_params=params(56),
        cost_estimate=COST["first"],
        name="first",
    )(counts, *sources, *weights)
    group = lax.all_to_all(group, ("y", "r"), 0, 0)
    feats_out = (TGT, TILES, ROWS, LANES)
    pos_out = (ROWS, LANES)
    feats, pos = pl.pallas_call(
        spread_kernel,
        out_shape=(jax.ShapeDtypeStruct(feats_out, BF16), jax.ShapeDtypeStruct(pos_out, BF16)),
        in_specs=[vmem],
        out_specs=(vmem, vmem),
        compiler_params=params(32),
        cost_estimate=COST["spread"],
        name="spread",
    )(group)
    feats = lax.all_to_all(feats, "tgt", 0, 0)
    zones = [pos]
    for shift in range(1, ZH):
        zones.append(lax.ppermute(pos, "zh", [(i, (i + shift) % ZH) for i in range(ZH)]))

    parts_out = (SRC, 4, ROWS, LANES)
    parts = pl.pallas_call(
        main_kernel,
        out_shape=jax.ShapeDtypeStruct(parts_out, BF16),
        in_specs=[hbm, vmem, vmem],
        out_specs=vmem,
        scratch_shapes=[
            pltpu.VMEM(((SLICES + 1) * ROWS, LANES), F32),
            pltpu.VMEM(((SLICES + 1) * ROWS, LANES), F32),
            pltpu.VMEM((17, (SLICES + 1) * ROWS, LANES), F32),
            pltpu.VMEM((SLICES, COLS, TGT * ROWS), BF16),
            pltpu.VMEM((COLS, 2 * STEP), F32),
            pltpu.VMEM((COLS, 2 * STEP), BF16),
            pltpu.VMEM((SRC * ROWS, 4 * LANES), F32),
            pltpu.SMEM((SLICES * (slots // STEP) + 5,), jnp.int32),
            pltpu.SMEM(counts.shape, jnp.int32),
            pltpu.SemaphoreType.DMA,
        ],
        compiler_params=params(32),
        cost_estimate=COST["edge_sums"],
        name="edge_sums",
    )(counts, feats, group)
    parts = pl.pallas_call(
        message_kernel,
        out_shape=jax.ShapeDtypeStruct(parts_out, BF16),
        in_specs=[vmem] * 8,
        out_specs=vmem,
        compiler_params=params(32),
        cost_estimate=COST["message"],
        input_output_aliases={7: 0},
        name="message",
    )(feats, *zones, k_index, k_filter, parts)
    parts = lax.all_to_all(parts, SRC_AXES, 0, 0)

    norm = 1.0 / math.sqrt(SRC * TGT * ROWS * k_index.shape[1])
    return pl.pallas_call(
        lambda *refs: last_conv_kernel(norm, *refs),
        out_shape=(
            jax.ShapeDtypeStruct((ROWS, columns), BF16),
            jax.ShapeDtypeStruct((ROWS, LANES), F32),
        ),
        in_specs=[vmem] * 6,
        out_specs=(vmem, vmem),
        scratch_shapes=[pltpu.VMEM((ROWS, columns), F32)],
        compiler_params=params(16),
        cost_estimate=COST["last_conv"],
        name="last_conv",
    )(parts, *weights)


def solution(mesh):
    fine = Mesh(mesh.devices.reshape(Y, ZH, R, TGT), ALL_AXES)
    return jax.shard_map(
        body,
        mesh=fine,
        in_specs=(P(ALL_AXES, None), P(None, ALL_AXES)) + (P(ALL_AXES),) * 4 + (P(),) * 8,
        out_specs=(P(("tgt",) + SRC_AXES, None), P(ALL_AXES, None)),
        check_vma=False,
    )
```
